32 devices in a mesh: prow: 4 (over z), pcol: 8 (over y, x, core).
Axes of the slice: x: 2, y: 2, z: 4, core: 2. Of those that a mesh axis runs over, the one named last changes fastest.
Arguments:
- points: float32 [1, 8, 2, 1024], P(None, 'pcol'), may hold values from 0 to 1
- range_length: float32 [1], replicated, may hold values from 0.05 to 0.15
- smoothness: int32 [1], replicated, may hold values from 0 to 2
- sketch_bank: bfloat16 [8, 48, 1024], P('pcol'), may hold values from -6 to 6
- sketch_ids: int32 [2, 4, 1, 8], P(None, 'prow', None, 'pcol'), may hold values from 0 to 7
- tile_ranks: int32 [2, 4, 1, 8], P(None, 'prow', None, 'pcol'), may hold values from 16 to 48
Outputs:
- y_factors: float32 [2, 4, 1, 8, 48, 1024], P(None, 'prow', None, 'pcol')
- c_factors: float32 [2, 4, 1, 8, 48, 1024], P(None, 'prow', None, 'pcol')
- tile_error: float32 [2, 4, 1, 8], P(None, 'prow', None, 'pcol')
- rank_total: int32 [1], replicated
The draws below stay inside these ranges and needn't reach their ends.
All inputs are finite; a program needn't handle non-finite values.
Results may differ from the reference program's by a relative error of at most 0.0098.
The reference program's roundings to bfloat16 on the way count: a program that leaves them out, or rounds other values in their place, can miss the bound.
Values may be sent and summed in bfloat16 or wider, within the bound.
A program may use at most 64 MiB of HBM per device.

```python
import math
import jax
import jax.numpy as jnp
import numpy as np
from jax import lax

NB = 1024
RMAX = 48
RMIN = 16
MTB = 1
MT = 8
TRD = 2
SB = 8
N_PROW = 4
N_PCOL = 8


def draw_points(key, part):
    total_bits = max(1, (MT - 1).bit_length())
    x_bits = (total_bits + 1) // 2
    y_bits = total_bits // 2
    blocks = jnp.arange(MT, dtype=jnp.int32)
    cell_x = jnp.zeros((MT,), jnp.float32)
    cell_y = jnp.zeros((MT,), jnp.float32)
    for level in range(total_bits):
        digit = (blocks // 2 ** level % 2).astype(jnp.float32)
        if level % 2 == 0:
            cell_x = cell_x + digit * float(2 ** (level // 2))
        else:
            cell_y = digit
    key_jitter = jax.random.fold_in(key, 11)
    key_spread = jax.random.fold_in(key, 23)
    key_select = jax.random.fold_in(key, 37)
    jitter = jax.random.uniform(key_jitter, (MT, 2, NB), jnp.float32)
    spread = jax.random.uniform(key_spread, (MT, 2, NB), jnp.float32)
    select = jax.random.uniform(key_select, (MT, 1, NB), jnp.float32)
    share = 0.25
    coord_x = (cell_x[:, None] + jitter[:, 0]) / float(2 ** x_bits)
    coord_y = (cell_y[:, None] + jitter[:, 1]) / float(2 ** y_bits)
    local = jnp.stack([coord_x, coord_y], axis=1)
    placed = jnp.where(select < share, spread, local)
    return placed.reshape(MTB, N_PCOL, 2, NB)


def plant(drawn, key, low, largest):
    longest = drawn.shape.index(max(drawn.shape))
    spots = []
    for shift in (0, 1):
        where = [jax.random.randint(jax.random.fold_in(key, axis), (), 0, length) for axis, length in enumerate(drawn.shape)]
        where[longest] = (where[longest] + shift) % drawn.shape[longest]
        spots.append(tuple(where))
    return drawn.at[spots[0]].set(low).at[spots[1]].set(largest)


def block_levels(stream_key, extent, shards, least, high):
    def one(axis_at, parts):
        heights = jax.random.uniform(jax.random.fold_in(jax.random.fold_in(stream_key, 6), axis_at), (parts,), jnp.float32, least / len(shards), high / len(shards))
        return jnp.repeat(jnp.exp(heights), extent[axis_at] // parts).reshape((-1,) + (1,) * (len(extent) - axis_at - 1))

    gain = one(*shards[0])
    for cut in shards[1:]:
        gain = gain * one(*cut)
    return gain


def noise(rng, shape, scale, reach, cuts=(), held_as=jnp.bfloat16):
    entries = scale * jax.random.normal(rng, shape, jnp.float32)
    if cuts:
        entries = entries * block_levels(rng, shape, cuts, -0.22, 0.18)
    return jnp.clip(entries, -reach, reach).astype(held_as)


def setup_inputs(seed: int = 0) -> dict:
    key_list = jax.random.split(jax.random.key(seed), 7)
    points = draw_points(jax.random.fold_in(key_list[6], 71), 0)
    range_length = jnp.clip(jnp.exp(jax.random.uniform(key_list[1], (1,), jnp.float32, math.log(0.05), math.log(0.15))), 0.05, 0.15)
    smoothness = jax.random.randint(key_list[2], (1,), 0, 3).astype(jnp.int32)
    sketch_bank = noise(key_list[3], (SB, RMAX, NB), 1.0, 6.0, ((0, 8),))
    sketch_ids = plant(jax.random.randint(key_list[4], (TRD, N_PROW, MTB, N_PCOL), 0, SB), jax.random.fold_in(key_list[4], 1), 0, SB - 1).astype(jnp.int32)
    tile_ranks = plant(jax.random.randint(key_list[5], (TRD, N_PROW, MTB, N_PCOL), RMIN, RMAX + 1), jax.random.fold_in(key_list[5], 1), RMIN, RMAX).astype(jnp.int32)
    return dict(points=points, range_length=range_length, smoothness=smoothness, sketch_bank=sketch_bank, sketch_ids=sketch_ids, tile_ranks=tile_ranks)


def kernel_factors(smoothness, range_length):
    morton_value = smoothness[0].astype(jnp.float32)
    kernel_scale = jnp.sqrt(2.0 * morton_value + 1.0) / range_length[0]
    linear_factor = jnp.where(smoothness[0] >= 1, 1.0, 0.0).astype(jnp.float32)
    squared_distance = jnp.where(smoothness[0] >= 2, 1.0 / 3.0, 0.0).astype(jnp.float32)
    return (kernel_scale, linear_factor, squared_distance)

def covariance_tile(row_locations, column_locations, kernel_scale, linear_factor, squared_distance):
    offset_horizontal = row_locations[0][:, None] - column_locations[0][None, :]
    offset_vertical = row_locations[1][:, None] - column_locations[1][None, :]
    scaled_distance = kernel_scale * jnp.sqrt(offset_horizontal * offset_horizontal + offset_vertical * offset_vertical)
    return (1.0 + linear_factor * scaled_distance + squared_distance * scaled_distance * scaled_distance) * jnp.exp(-scaled_distance)

def compress(tile_low, sketch, rank):
    keep = jnp.arange(sketch.shape[0]) < rank
    sketch = jnp.where(keep[:, None], sketch, jnp.zeros_like(sketch))
    sketched = lax.dot_general(sketch.astype(jnp.float32), tile_low.astype(jnp.float32), (((1,), (1,)), ((), ())), preferred_element_type=jnp.float32)
    product = jnp.dot(sketched.astype(jnp.bfloat16).astype(jnp.float32), tile_low.astype(jnp.float32), preferred_element_type=jnp.float32)
    gram = jnp.dot(sketched, sketched.T, precision=lax.Precision.HIGHEST)
    shift = 0.1 * jnp.trace(gram) / rank.astype(jnp.float32)
    gram = gram + jnp.diag(jnp.where(keep, shift, jnp.ones_like(shift)))
    factor = jnp.linalg.cholesky(gram)
    coeffs = jax.scipy.linalg.cho_solve((factor, True), product)
    approx = lax.dot_general(sketched, coeffs, (((0,), (0,)), ((), ())), precision=lax.Precision.HIGHEST)
    error = tile_low.astype(jnp.float32) - approx
    return (sketched, coeffs, jnp.sum(error * error))

def reference(points, range_length, smoothness, sketch_bank, sketch_ids, tile_ranks):
    every_block = points.reshape(MT, 2, NB)
    kernel_scale, linear_factor, squared_distance = kernel_factors(smoothness, range_length)
    pairs = np.array([(row, col) for row in range(MT) for col in range(row + 1)], np.int32)
    row_index = jnp.asarray(pairs[:, 0]).astype(jnp.int32)
    col_index = jnp.asarray(pairs[:, 1]).astype(jnp.int32)
    row_major = row_index // N_PROW
    row_minor = row_index % N_PROW
    col_major = col_index // N_PCOL
    col_minor = col_index % N_PCOL
    chosen_ids = sketch_ids[row_major, row_minor, col_major, col_minor]
    chosen_ranks = tile_ranks[row_major, row_minor, col_major, col_minor]

    def one_tile(inputs):
        row_number, column_number, sketch_id, rank = inputs
        tile_block = covariance_tile(every_block[row_number], every_block[column_number], kernel_scale, linear_factor, squared_distance)
        norm_sq = jnp.sum(tile_block * tile_block)
        tile_low = tile_block.astype(jnp.bfloat16)
        sketched, coeffs, err_sq = compress(tile_low, sketch_bank[sketch_id], rank)
        return (sketched, coeffs, norm_sq, err_sq)
    sketched_all, coeffs_all, norm_all, err_all = lax.map(one_tile, (row_index, col_index, chosen_ids, chosen_ranks))
    offdiag = row_index > col_index
    total = jnp.sum(jnp.where(offdiag, 2.0, 1.0) * norm_all)
    errors = jnp.where(offdiag, jnp.sqrt(err_all), jnp.sqrt(norm_all)) * MT / jnp.sqrt(total)
    shape_out = (TRD, N_PROW, MTB, N_PCOL, RMAX, NB)
    y_out = jnp.zeros(shape_out, jnp.float32).at[row_major, row_minor, col_major, col_minor].set(jnp.where(offdiag[:, None, None], sketched_all, 0.0))
    c_out = jnp.zeros(shape_out, jnp.float32).at[row_major, row_minor, col_major, col_minor].set(jnp.where(offdiag[:, None, None], coeffs_all, 0.0))
    err_out = jnp.zeros((TRD, N_PROW, MTB, N_PCOL), jnp.float32).at[row_major, row_minor, col_major, col_minor].set(errors)
    rank_out = jnp.sum(jnp.where(offdiag, chosen_ranks, 0)).astype(jnp.int32).reshape(1)
    return (y_out, c_out, err_out, rank_out)
```

```python
import functools
import math

import jax
import jax.numpy as jnp
from jax import lax
from jax.experimental import pallas as pl
from jax.experimental.pallas import tpu as pltpu
from jax.sharding import PartitionSpec as P

MESH = pl.DeviceIdType.MESH
LOG2E = math.log2(math.e)
F32 = jnp.float32
BF16 = jnp.bfloat16
HIGH = lax.Precision.HIGHEST


def dot(a, b, da, db, precision=None):
    return lax.dot_general(
        a, b, (((da,), (db,)), ((), ())), preferred_element_type=F32, precision=precision
    )


def split(x):
    high = x.astype(BF16)
    return high, (x - high.astype(F32)).astype(BF16)


def all_sum(x):
    return jnp.sum(jnp.sum(x, axis=1, keepdims=True), axis=0, keepdims=True)


def invert(m, size, half, group=8):
    parts = size // 8
    width = m.shape[1]
    sub = lax.broadcasted_iota(jnp.int32, (8, width), 0)
    lane = lax.broadcasted_iota(jnp.int32, (8, width), 1)
    side = lane // half * half
    lane = lane - side
    m = [m[8 * v : 8 * v + 8] for v in range(parts)]
    for start in range(0, size, group):
        cols = {
            k: [jnp.take_along_axis(part, side + k, axis=1) for part in m]
            for k in range(start, start + group)
        }
        for k in range(start, start + group):
            at, within = divmod(k, 8)
            col = cols.pop(k)
            pivot = jnp.broadcast_to(col[at][within : within + 1], (8, width))
            inverse = 1.0 / pivot
            for other, entry in cols.items():
                head = jnp.broadcast_to(entry[at][within : within + 1], (8, width)) * inverse
                entry = [e - c * head for e, c in zip(entry, col)]
                entry[at] = jnp.where(sub == within, head, entry[at])
                cols[other] = entry
            row = jnp.broadcast_to(m[at][within : within + 1], (8, width))
            row = jnp.where(lane == k, 1.0, row) * inverse
            m = [jnp.where(lane == k, 0.0, part) - c * row for part, c in zip(m, col)]
            m[at] = jnp.where(sub == within, row, m[at])
    return jnp.concatenate(m, axis=0)


def fold(x):
    rows, width = x.shape
    x = jnp.sum(x.reshape(rows // 8, 8, width), axis=0)
    return functools.reduce(jnp.add, [x[:, n : n + 128] for n in range(0, width, 128)])


def kernel(
    rows,
    cols,
    row_tiles,
    col_tiles,
    range_length,
    smoothness,
    points_hbm,
    bank_hbm,
    ids_hbm,
    ranks_hbm,
    y_out,
    c_out,
    residuals,
    whole_out,
    ids,
    ranks,
    all_points,
    all_bank,
    low,
    norms,
    y_pair,
    w_pair,
    mine,
    sums,
    sem_local,
    sem_ps,
    sem_pr,
    sem_bs,
    sem_br,
    sem_sr,
    sem_ns,
    sem_nr,
    ready,
):
    p = lax.axis_index("prow")
    q = lax.axis_index("pcol")
    per_bank, sketch_rows, size = bank_hbm.shape
    slots = [(a, b) for a in range(row_tiles) for b in range(col_tiles)]
    sibling = q + 1 - 2 * lax.rem(q, 2)

    barrier = pltpu.get_barrier_semaphore()
    for step in range(1, cols):
        pl.semaphore_signal(
            barrier, device_id=(p, lax.rem(q + step, cols)), device_id_type=MESH
        )
    for step in range(1, rows):
        pl.semaphore_signal(
            barrier, device_id=(lax.rem(p + step, rows), q), device_id_type=MESH
        )
    own_bank = pl.ds(q * per_bank, per_bank)
    local = [
        pltpu.make_async_copy(source, target, sem_local.at[index])
        for index, (source, target) in enumerate(
            [
                (points_hbm.at[:, 0], all_points.at[q]),
                (bank_hbm, all_bank.at[own_bank]),
                (ids_hbm, ids),
                (ranks_hbm, ranks),
            ]
        )
    ]
    for copy in local:
        copy.start()
    needed = q < 0
    for a in range(row_tiles):
        needed = needed | (lax.rem(a * rows + p, cols) == q)
    y_pair[...] = jnp.zeros_like(y_pair)
    w_pair[...] = jnp.zeros_like(w_pair)
    for copy in local:
        copy.wait()
    pl.semaphore_wait(barrier, cols + rows - 2)
    for step in range(1, rows):
        pl.semaphore_signal(
            ready, device_id=(lax.rem(p + step, rows), q), device_id_type=MESH
        )

    def point_copy(source, target):
        return pltpu.make_async_remote_copy(
            src_ref=all_points.at[source],
            dst_ref=all_points.at[source],
            send_sem=sem_ps,
            recv_sem=sem_pr.at[source],
            device_id=(p, target),
            device_id_type=MESH,
        )

    def bank_copy(block, target, recv, count=1):
        at = pl.ds(block * per_bank, per_bank * count)
        return pltpu.make_async_remote_copy(
            src_ref=all_bank.at[at],
            dst_ref=all_bank.at[at],
            send_sem=sem_bs,
            recv_sem=recv,
            device_id=(p, target),
            device_id_type=MESH,
        )

    @pl.when(needed)
    def _():
        for step in range(1, cols):
            point_copy(q, lax.rem(q + step, cols)).start()

    for step in range(2, cols, 2):
        bank_copy(q, lax.rem(q + step, cols), sem_br.at[q]).start()
    bank_copy(q, sibling, sem_sr).start()

    degree = jnp.full((8, 128), smoothness[0].astype(F32))
    scale = (LOG2E * jnp.sqrt(2.0 * degree + 1.0)) / jnp.full((8, 128), range_length[0])
    scale = scale[:1]
    linear = jnp.where(smoothness[0] >= 1, 1.0 / LOG2E, 0.0).astype(F32)
    square = jnp.where(smoothness[0] >= 2, 1.0 / (3.0 * LOG2E * LOG2E), 0.0).astype(F32)

    def place(slot):
        a, b = slots[slot]
        return a * rows + p, b * cols + q

    arrived = []

    def generate(slot, begin=0, end=size // 128):
        i, j = place(slot)
        a = slots[slot][0]
        owner = lax.rem(a * rows + p, cols)
        fresh = owner != q
        for before in arrived:
            if before != a:
                fresh = fresh & (owner != lax.rem(before * rows + p, cols))
        if a not in arrived and begin == 0:
            arrived.append(a)

            @pl.when(fresh)
            def _():
                point_copy(owner, q).wait_recv()

        @pl.when(j > i)
        def _():
            norms[slot] = jnp.zeros((8, 128), F32)

            def clear(c, _):
                low[slot, pl.ds(pl.multiple_of(c * 128, 128), 128)] = jnp.zeros((128, size), BF16)
                return 0

            lax.fori_loop(begin, end, clear, 0)

        @pl.when(j <= i)
        def _():
            row_block = lax.rem(i, cols)
            row_major = i // cols
            col_major = slots[slot][1]

            def chunk(c, total):
                at = pl.ds(pl.multiple_of(c * 128, 128), 128)
                x_row = all_points[row_block, row_major, 0:1, at] * scale
                y_row = all_points[row_block, row_major, 1:2, at] * scale
                x_row = jnp.broadcast_to(x_row, (128, 128)).T
                y_row = jnp.broadcast_to(y_row, (128, 128)).T
                for n in range(size // 128):
                    cut = slice(n * 128, n * 128 + 128)
                    x_col = all_points[q, col_major, 0:1, cut] * scale
                    y_col = all_points[q, col_major, 1:2, cut] * scale
                    dx = x_row - x_col
                    dy = y_row - y_col
                    d2 = dx * dx + dy * dy
                    t = d2 * lax.rsqrt(jnp.maximum(d2, 1e-30))
                    tile = ((1.0 + linear * t + square * d2) * jnp.exp2(-t)).astype(BF16)
                    low[slot, at, cut] = tile
                    tile = tile.astype(F32)
                    total = total + jnp.sum((tile * tile).reshape(16, 8, 128), axis=0)
                return total

            total = jnp.zeros((8, 128), F32) if begin == 0 else norms[slot]
            norms[slot] = lax.fori_loop(begin, end, chunk, total)

    for slot in range(len(slots) - 1):
        generate(slot)
    split_at = size // 256
    generate(len(slots) - 1, 0, split_at)
    for step in range(2, cols, 2):
        block = lax.rem(q + step, cols)
        bank_copy(block, q, sem_br.at[block]).wait_recv()
        bank_copy(block, sibling, sem_sr).start()
    generate(len(slots) - 1, split_at)

    devices = rows * cols
    me = p * cols + q

    def norm_copy(target):
        return pltpu.make_async_remote_copy(
            src_ref=mine,
            dst_ref=sums.at[me],
            send_sem=sem_ns,
            recv_sem=sem_nr,
            device_id=(target // cols, lax.rem(target, cols)),
            device_id_type=MESH,
        )

    norm_sum = jnp.zeros((8, 128), F32)
    rank_sum = jnp.float32(0)
    for slot, (a, b) in enumerate(slots):
        i, j = place(slot)
        norm_sum = norm_sum + jnp.where(j < i, 2.0, 1.0).astype(F32) * norms[slot]
        rank_sum = rank_sum + jnp.where(j < i, ranks[0, b, 0, a], 0).astype(F32)
    mine[0:1, :] = jnp.sum(norm_sum, axis=0, keepdims=True)
    mine[1:2, :] = jnp.full((1, 128), rank_sum)
    sums[me] = mine[...]

    pl.semaphore_wait(ready, rows - 1)
    for step in range(1, devices):
        norm_copy(lax.rem(me + step, devices)).start()

    bank_copy(0, q, sem_sr, cols // 2).wait_recv()

    half = 64
    row_at = lax.broadcasted_iota(jnp.int32, (sketch_rows, 1), 0)

    def rank_of(slot):
        a, b = slots[slot]
        i, j = place(slot)
        return jnp.where(j < i, ranks[0, b, 0, a], 0)

    for first in range(0, len(slots), 2):
        pair = list(enumerate(range(first, min(first + 2, len(slots)))))
        products = []
        for side, slot in pair:
            a, b = slots[slot]
            sketch = all_bank[ids[0, b, 0, a]]
            sketch = jnp.where(row_at < rank_of(slot), sketch.astype(F32), 0.0).astype(BF16)
            y = dot(sketch, low[slot], 1, 1)
            y_out[a, 0, b, 0] = y
            y_pair[side * half : side * half + sketch_rows] = y
        for side, slot in pair:
            a, b = slots[slot]
            product = dot(jnp.concatenate(split(y_out[a, 0, b, 0]), axis=0), low[slot], 1, 0)
            w_pair[side * half : side * half + sketch_rows] = product[:sketch_rows]
            products.append(product[:sketch_rows] + 2.0 * product[sketch_rows:])
        gram = dot(y_pair[...], y_pair[...], 1, 1, HIGH)
        lane = lax.broadcasted_iota(jnp.int32, (sketch_rows, 2 * half), 1)
        sub = lax.broadcasted_iota(jnp.int32, (sketch_rows, 2 * half), 0)
        left = lane < half
        gram = jnp.where(left, gram[:sketch_rows], gram[half : half + sketch_rows])
        eye = lane == jnp.where(left, sub, sub + half)
        shifts = []
        diagonal = jnp.ones((sketch_rows, 2 * half), F32)
        for side, slot in pair:
            a, b = slots[slot]
            mask = left if side == 0 else ~left
            rank = jnp.full((1, 1), ranks[0, b, 0, a].astype(F32))
            shift = 0.1 * all_sum(jnp.where(eye & mask, gram, 0.0)) / rank
            shifts.append(shift)
            diagonal = jnp.where(mask & (sub < rank_of(slot)), shift, diagonal)
        inverse = invert(gram + jnp.where(eye, diagonal, 0.0), sketch_rows, half)
        inverse = jnp.concatenate(
            [jnp.where(left if side == 0 else ~left, inverse, 0.0) for side, _ in pair], axis=0
        )
        coefficients = dot(inverse, w_pair[...], 1, 0, HIGH)
        for side, slot in pair:
            a, b = slots[slot]
            i, j = place(slot)
            c = coefficients[side * sketch_rows : (side + 1) * sketch_rows]
            c_out[a, 0, b, 0] = c
            gain = fold(c * (products[side] + shifts[side] * c))
            residuals[slot] = norms[slot] - jnp.where(j < i, gain, 0.0)

    def norm_wait(ref):
        return pltpu.make_async_remote_copy(
            src_ref=ref,
            dst_ref=ref,
            send_sem=sem_ns,
            recv_sem=sem_nr,
            device_id=(p, sibling),
            device_id_type=MESH,
        )

    others = norm_wait(sums.at[pl.ds(0, devices - 1)])
    others.wait_recv()
    whole_out[...] = jnp.sum(sums[...], axis=0)
    others.wait_send()

    @pl.when(needed)
    def _():
        pltpu.make_async_remote_copy(
            src_ref=all_points.at[pl.ds(0, cols - 1)],
            dst_ref=all_points.at[pl.ds(0, cols - 1)],
            send_sem=sem_ps,
            recv_sem=sem_pr.at[0],
            device_id=(p, sibling),
            device_id_type=MESH,
        ).wait_send()

    bank_copy(0, sibling, sem_sr, cols - 1).wait_send()


def finish(rows, cols, row_tiles, col_tiles, y, c, residuals, whole, y_out, c_out, err_out, rank_out, sems):
    p = lax.axis_index("prow")
    q = lax.axis_index("pcol")
    copies = [
        pltpu.make_async_copy(source.at[a], target.at[a], sems.at[index, a])
        for index, (source, target) in enumerate([(y, y_out), (c, c_out)])
        for a in range(row_tiles)
    ]
    for copy in copies:
        copy.start()
    norm = lax.rsqrt(all_sum(whole[0:1, :])) * float(cols * col_tiles)
    lane = lax.broadcasted_iota(jnp.int32, (1, 128), 1)
    for b in range(col_tiles):
        line = jnp.zeros((1, 128), F32)
        for a in range(row_tiles):
            error = jnp.sqrt(jnp.maximum(all_sum(residuals[a * col_tiles + b]), 0.0)) * norm
            shown = (lane == a) & (b * cols + q <= a * rows + p)
            line = jnp.where(shown, error, line)
        err_out[0, b, 0:1, :] = line[:, :row_tiles]
    rank_out[0] = whole[1:2, 0:1].astype(jnp.int32)[0, 0]
    for copy in copies:
        copy.wait()


def per_device(rows, cols, points, range_length, smoothness, bank, ids, ranks):
    row_tiles, col_tiles = ids.shape[0], ids.shape[2]
    per_bank, sketch_rows, size = bank.shape
    slots = row_tiles * col_tiles
    ids = ids.transpose(1, 2, 3, 0)
    ranks = ranks.transpose(1, 2, 3, 0)
    factors = jax.ShapeDtypeStruct((row_tiles, 1, col_tiles, 1, sketch_rows, size), F32)
    vmem = pl.BlockSpec(memory_space=pltpu.VMEM)
    smem = pl.BlockSpec(memory_space=pltpu.SMEM)
    hbm = pl.BlockSpec(memory_space=pltpu.HBM)
    dma = pltpu.SemaphoreType.DMA
    pinned = [pltpu.with_memory_space_constraint(x, pltpu.HBM) for x in (points, bank, ids, ranks)]
    y, c, residuals, whole = pl.pallas_call(
        functools.partial(kernel, rows, cols, row_tiles, col_tiles),
        out_shape=(
            factors,
            factors,
            jax.ShapeDtypeStruct((slots, 8, 128), F32),
            jax.ShapeDtypeStruct((2, 128), F32),
        ),
        in_specs=[smem, smem, hbm, hbm, hbm, hbm],
        out_specs=(vmem,) * 4,
        scratch_shapes=[
            pltpu.SMEM(ids.shape, jnp.int32),
            pltpu.SMEM(ranks.shape, jnp.int32),
            pltpu.VMEM((cols, col_tiles, 2, size), F32),
            pltpu.VMEM((cols * per_bank, sketch_rows, size), BF16),
            pltpu.VMEM((slots, size, size), BF16),
            pltpu.VMEM((slots, 8, 128), F32),
            pltpu.VMEM((128, size), F32),
            pltpu.VMEM((128, size), F32),
            pltpu.VMEM((2, 128), F32),
            pltpu.VMEM((rows * cols, 2, 128), F32),
            dma((4,)),
            dma,
            dma((cols,)),
            dma,
            dma((cols,)),
            dma,
            dma,
            dma,
            pltpu.SemaphoreType.REGULAR,
        ],
        compiler_params=pltpu.CompilerParams(
            collective_id=0, has_side_effects=True, vmem_limit_bytes=40 * 1024 * 1024
        ),
        name="tiles",
    )(range_length, smoothness, *pinned)
    y, c, errors, rank_total = pl.pallas_call(
        functools.partial(finish, rows, cols, row_tiles, col_tiles),
        out_shape=(
            factors,
            factors,
            jax.ShapeDtypeStruct((1, col_tiles, 1, row_tiles), F32),
            jax.ShapeDtypeStruct((1,), jnp.int32),
        ),
        in_specs=[vmem] * 4,
        out_specs=(hbm, hbm, vmem, smem),
        scratch_shapes=[dma((2, row_tiles))],
        compiler_params=pltpu.CompilerParams(vmem_limit_bytes=16 * 1024 * 1024),
        name="finish",
    )(y, c, residuals, whole)
    return y, c, errors.transpose(3, 0, 1, 2), rank_total


def solution(mesh):
    in_specs = (
        P(None, "pcol", None, None),
        P(),
        P(),
        P("pcol", None, None),
        P(None, "prow", None, "pcol"),
        P(None, "prow", None, "pcol"),
    )
    out_specs = (
        P(None, "prow", None, "pcol", None, None),
        P(None, "prow", None, "pcol", None, None),
        P(None, "prow", None, "pcol"),
        P(),
    )
    return jax.shard_map(
        functools.partial(per_device, mesh.shape["prow"], mesh.shape["pcol"]),
        mesh=mesh,
        in_specs=in_specs,
        out_specs=out_specs,
        check_vma=False,
    )
```

```python
import functools
import math

import jax
import jax.numpy as jnp
from jax import lax
from jax.experimental import pallas as pl
from jax.experimental.pallas import tpu as pltpu
from jax.sharding import PartitionSpec as P

MESH = pl.DeviceIdType.MESH
LOG2E = math.log2(math.e)
F32 = jnp.float32
BF16 = jnp.bfloat16
HIGH = lax.Precision.HIGHEST


def dot(a, b, da, db, precision=None):
    return lax.dot_general(
        a, b, (((da,), (db,)), ((), ())), preferred_element_type=F32, precision=precision
    )


def split(x):
    high = x.astype(BF16)
    return high, (x - high.astype(F32)).astype(BF16)


def all_sum(x):
    return jnp.sum(jnp.sum(x, axis=1, keepdims=True), axis=0, keepdims=True)


def invert(m, size, half, group=8):
    parts = size // 8
    width = m.shape[1]
    sub = lax.broadcasted_iota(jnp.int32, (8, width), 0)
    lane = lax.broadcasted_iota(jnp.int32, (8, width), 1)
    side = lane // half * half
    lane = lane - side
    m = [m[8 * v : 8 * v + 8] for v in range(parts)]
    for start in range(0, size, group):
        cols = {
            k: [jnp.take_along_axis(part, side + k, axis=1) for part in m]
            for k in range(start, start + group)
        }
        for k in range(start, start + group):
            at, within = divmod(k, 8)
            col = cols.pop(k)
            pivot = jnp.broadcast_to(col[at][within : within + 1], (8, width))
            inverse = 1.0 / pivot
            for other, entry in cols.items():
                head = jnp.broadcast_to(entry[at][within : within + 1], (8, width)) * inverse
                entry = [e - c * head for e, c in zip(entry, col)]
                entry[at] = jnp.where(sub == within, head, entry[at])
                cols[other] = entry
            row = jnp.broadcast_to(m[at][within : within + 1], (8, width))
            row = jnp.where(lane == k, 1.0, row) * inverse
            m = [jnp.where(lane == k, 0.0, part) - c * row for part, c in zip(m, col)]
            m[at] = jnp.where(sub == within, row, m[at])
    return jnp.concatenate(m, axis=0)


def fold(x):
    rows, width = x.shape
    x = jnp.sum(x.reshape(rows // 8, 8, width), axis=0)
    return functools.reduce(jnp.add, [x[:, n : n + 128] for n in range(0, width, 128)])


def kernel(
    rows,
    cols,
    row_tiles,
    col_tiles,
    range_length,
    smoothness,
    points_hbm,
    bank_hbm,
    ids_hbm,
    ranks_hbm,
    y_out,
    c_out,
    residuals,
    whole_out,
    ids,
    ranks,
    all_points,
    all_bank,
    low,
    norms,
    x_spread,
    y_spread,
    line,
    mine,
    sums,
    sem_local,
    sem_ps,
    sem_pr,
    sem_bs,
    sem_br,
    sem_sr,
    sem_ns,
    sem_nr,
    ready,
):
    p = lax.axis_index("prow")
    q = lax.axis_index("pcol")
    per_bank, sketch_rows, size = bank_hbm.shape
    slots = [(a, b) for a in range(row_tiles) for b in range(col_tiles)]
    sibling = q + 1 - 2 * lax.rem(q, 2)
    mirrored = row_tiles == 2 and col_tiles == 1 and cols == 2 * rows

    barrier = pltpu.get_barrier_semaphore()
    for step in range(1, cols):
        pl.semaphore_signal(
            barrier, device_id=(p, lax.rem(q + step, cols)), device_id_type=MESH
        )
    gate = q == 0

    def tell_gates(semaphore):
        for step in range(1, rows):
            pl.semaphore_signal(
                semaphore, device_id=(lax.rem(p + step, rows), 0), device_id_type=MESH
            )

    @pl.when(gate)
    def _():
        tell_gates(barrier)

    own_bank = pl.ds(q * per_bank, per_bank)
    local = [
        pltpu.make_async_copy(source, target, sem_local.at[index])
        for index, (source, target) in enumerate(
            [
                (points_hbm.at[:, 0], all_points.at[q]),
                (bank_hbm, all_bank.at[own_bank]),
                (ids_hbm, ids),
                (ranks_hbm, ranks),
            ]
        )
    ]
    for copy in local:
        copy.start()
    def place(slot):
        a, b = slots[slot]
        return a * rows + p, b * cols + q

    def wants_bank(device):
        wanted = device < 0
        for a, b in slots:
            wanted = wanted | (b * cols + device < a * rows + p)
        return wanted

    def wants_points(source, target):
        if mirrored:
            early = (source == p) & ((target < p) | (target >= p + rows))
            return early | ((source == p + rows) & (target < source))
        wanted = source < 0
        for a in range(row_tiles):
            wanted = wanted | (lax.rem(a * rows + p, cols) == source)
        return wanted

    bank_steps = []
    for step in range(cols - 2, 0, -2):
        other = lax.rem(q + step, cols)
        twin = other + 1 - 2 * lax.rem(other, 2)
        bank_steps.append((other, wants_bank(other) | wants_bank(twin)))
    here, beside = wants_bank(q), wants_bank(sibling)

    def clear(slot):
        norms[slot] = jnp.zeros((8, 128), F32)

        def chunk(c, _):
            low[slot, pl.ds(pl.multiple_of(c * 128, 128), 128)] = jnp.zeros((128, size), BF16)
            return 0

        lax.fori_loop(0, size // 128, chunk, 0)

    for slot in range(len(slots)):
        i, j = place(slot)
        pl.when(j > i)(functools.partial(clear, slot))
    for copy in local:
        copy.wait()

    def point_copy(source, target):
        return pltpu.make_async_remote_copy(
            src_ref=all_points.at[source],
            dst_ref=all_points.at[source],
            send_sem=sem_ps,
            recv_sem=sem_pr.at[source],
            device_id=(p, target),
            device_id_type=MESH,
        )

    def bank_copy(block, target, recv, count=1):
        at = pl.ds(block * per_bank, per_bank * count)
        return pltpu.make_async_remote_copy(
            src_ref=all_bank.at[at],
            dst_ref=all_bank.at[at],
            send_sem=sem_bs,
            recv_sem=recv,
            device_id=(p, target),
            device_id_type=MESH,
        )

    degree = jnp.full((8, 128), smoothness[0].astype(F32))
    scale = (LOG2E * jnp.sqrt(2.0 * degree + 1.0)) / jnp.full((8, 128), range_length[0])
    scale = scale[:1]
    linear, square = 1.0 / LOG2E, 1.0 / (3.0 * LOG2E * LOG2E)

    def by_order(zero, one, two):
        return jnp.where(smoothness[0] >= 2, two, jnp.where(smoothness[0] >= 1, one, zero)).astype(F32)

    offset = by_order(-38.0, -31.0, math.log2(square))
    first = by_order(0.0, linear * 2.0**31, linear / square)
    constant = by_order(2.0**38, 2.0**31, 1.0 / square)
    for b in range(col_tiles):
        for n in range(0, size, 128):
            cut = slice(n, n + 128)
            x_own = all_points[q, b, 0:1, cut] * scale
            y_own = all_points[q, b, 1:2, cut] * scale
            x_spread[b, cut] = jnp.broadcast_to(x_own, (128, 128)).T
            y_spread[b, cut] = jnp.broadcast_to(y_own, (128, 128)).T

    def generate(slot, begin=0, end=size // 128):
        i, j = place(slot)
        b = slots[slot][1]
        row_block, row_major = lax.rem(i, cols), i // cols
        for n in range(0, size, 128):
            cut = slice(n, n + 128)
            line[:, cut] = all_points[row_block, row_major, :, cut] * scale

        def chunk(c, total):
            at = pl.ds(pl.multiple_of(c * 128, 128), 128)
            x_own, y_own = x_spread[b, at], y_spread[b, at]
            for n in range(0, size, 128):
                cut = slice(n, n + 128)
                dx = x_own - line[0:1, cut]
                dy = y_own - line[1:2, cut]
                d2 = dx * dx + dy * dy
                t = d2 * lax.rsqrt(jnp.maximum(d2, 1e-30))
                tile = ((constant + t * (first + t)) * jnp.exp2(offset - t)).astype(BF16)
                low[slot, at, cut] = tile
                tile = tile.astype(F32)
                total = total + jnp.sum((tile * tile).reshape(16, 8, 128), axis=0)
            return total

        total = jnp.zeros((8, 128), F32) if begin == 0 else norms[slot]
        norms[slot] = lax.fori_loop(begin, end, chunk, total)

    i, j = place(0)
    pl.when((i == 0) & (j == 0))(functools.partial(generate, 0))

    pl.semaphore_wait(barrier, cols - 1 + jnp.where(gate, rows - 1, 0))

    point_targets = [lax.rem(q + cols - step, cols) for step in range(1, cols)]
    for target in point_targets:
        pl.when(wants_points(q, target))(point_copy(q, target).start)
    for other, wanted in bank_steps:
        pl.when(wanted)(bank_copy(q, other, sem_br.at[q]).start)
    pl.when(beside)(bank_copy(q, sibling, sem_sr).start)
    @pl.when(gate)
    def _():
        tell_gates(ready)

    def open_gate():
        pl.semaphore_wait(ready, rows - 1)
        for step in range(1, cols):
            pl.semaphore_signal(ready, device_id=(p, step), device_id_type=MESH)


    def forward():
        for other, _ in bank_steps:
            pl.when(here | beside)(bank_copy(other, q, sem_br.at[other]).wait_recv)
            pl.when(beside)(bank_copy(other, sibling, sem_sr).start)

    devices = rows * cols
    me = p * cols + q

    def norm_copy(target):
        return pltpu.make_async_remote_copy(
            src_ref=mine,
            dst_ref=sums.at[me],
            send_sem=sem_ns,
            recv_sem=sem_nr,
            device_id=(target // cols, lax.rem(target, cols)),
            device_id_type=MESH,
        )

    def send_norms(weights):
        norm_sum = jnp.zeros((8, 128), F32)
        rank_sum = jnp.float32(0)
        for slot, (a, b) in enumerate(slots):
            i, j = place(slot)
            norm_sum = norm_sum + weights[slot] * norms[slot]
            rank_sum = rank_sum + jnp.where(j < i, ranks[0, b, 0, a], 0).astype(F32)
        mine[0:1, :] = jnp.sum(norm_sum, axis=0, keepdims=True)
        mine[1:2, :] = jnp.full((1, 128), rank_sum)
        sums[me] = mine[...]
        pl.when(~gate)(functools.partial(pl.semaphore_wait, ready, 1))
        for step in range(1, devices):
            norm_copy(lax.rem(me + step, devices)).start()

    arrived = []

    def await_points(a):
        owner = lax.rem(a * rows + p, cols)
        fresh = owner != q
        for before in arrived:
            fresh = fresh & (owner != lax.rem(before * rows + p, cols))
        arrived.append(a)

        @pl.when(fresh & wants_points(owner, q))
        def _():
            point_copy(owner, q).wait_recv()

    if mirrored:
        middle = size // 256
        both, lone = q <= p, (q > p) & (q <= p + rows)
        pl.when(q == p + rows)(functools.partial(generate, 1))
        await_points(0)
        pl.when(gate & (p > 0))(functools.partial(generate, 0, 0, middle))
        pl.when(gate)(open_gate)
        pl.when(gate & (p > 0))(functools.partial(generate, 0, middle))
        pl.when((both & ~gate) | (q >= p + rows))(functools.partial(generate, 0))
        await_points(1)
        pl.when(lone & (q < p + rows))(functools.partial(generate, 1))
        from_first = jnp.where((q < p) | (q >= p + rows), 2.0, jnp.where(q == p, 1.0, 0.0))
        from_second = jnp.where(lone, jnp.where(q < p + rows, 2.0, 1.0), 0.0)
        send_norms([from_first, from_second])
        pl.when(both)(functools.partial(generate, 1, 0, middle))
        pl.when(q == p)(functools.partial(generate, 1, middle))
        forward()
        pl.when(q < p)(functools.partial(generate, 1, middle))
    else:
        for slot, (a, b) in enumerate(slots):
            i, j = place(slot)
            if a not in arrived:
                await_points(a)
            pl.when((j <= i) & (i + j > 0) if slot == 0 else j <= i)(functools.partial(generate, slot))
        pl.when(gate)(open_gate)
        weights = []
        for slot in range(len(slots)):
            i, j = place(slot)
            weights.append(jnp.where(j < i, 2.0, 1.0))
        send_norms(weights)
        forward()

    pl.when(here)(bank_copy(0, q, sem_sr, cols // 2).wait_recv)

    half = 64
    row_at = lax.broadcasted_iota(jnp.int32, (sketch_rows, 1), 0)

    def rank_of(slot):
        a, b = slots[slot]
        i, j = place(slot)
        return jnp.where(j < i, ranks[0, b, 0, a], 0)

    blank = jnp.zeros((half - sketch_rows, size), BF16)

    def stack(parts):
        full = [x for part in parts for x in (part, blank)]
        if len(parts) == 1:
            full += full[:1] + [blank]
        return jnp.concatenate(full, axis=0)

    for first in range(0, len(slots), 2):
        pair = list(enumerate(range(first, min(first + 2, len(slots)))))
        highs, lows = [], []
        for side, slot in pair:
            a, b = slots[slot]
            sketch = all_bank[ids[0, b, 0, a]]
            sketch = jnp.where(row_at < rank_of(slot), sketch.astype(F32), 0.0).astype(BF16)
            y = dot(sketch, low[slot], 1, 0)
            y_out[a, 0, b, 0] = y
            high, rest = split(y)
            highs.append(high)
            lows.append(rest)
        high, rest = stack(highs), stack(lows)
        gram = dot(jnp.concatenate([high, rest], axis=0), high, 1, 1)
        gram = gram[: 2 * half] + gram[2 * half :] + dot(high, rest, 1, 1)
        lane = lax.broadcasted_iota(jnp.int32, (sketch_rows, 2 * half), 1)
        sub = lax.broadcasted_iota(jnp.int32, (sketch_rows, 2 * half), 0)
        left = lane < half
        gram = jnp.where(left, gram[:sketch_rows], gram[half : half + sketch_rows])
        eye = lane == jnp.where(left, sub, sub + half)
        shifts = []
        diagonal = jnp.ones((sketch_rows, 2 * half), F32)
        for side, slot in pair:
            a, b = slots[slot]
            mask = left if side == 0 else ~left
            rank = jnp.full((1, 1), ranks[0, b, 0, a].astype(F32))
            shift = 0.1 * all_sum(jnp.where(eye & mask, gram, 0.0)) / rank
            shifts.append(shift)
            diagonal = jnp.where(mask & (sub < rank_of(slot)), shift, diagonal)
        inverse = invert(gram + jnp.where(eye, diagonal, 0.0), sketch_rows, half)
        products, highs_w, lows_w = [], [], []
        for side, slot in pair:
            product = dot(jnp.concatenate([highs[side], lows[side]], axis=0), low[slot], 1, 1)
            high, rest = split(product[:sketch_rows])
            highs_w.append(high)
            lows_w.append(rest)
            products.append(product[:sketch_rows] + 2.0 * product[sketch_rows:])
        weights = jnp.concatenate([stack(highs_w), stack(lows_w)], axis=0)
        sides = [jnp.where(left if side == 0 else ~left, inverse, 0.0) for side, _ in pair]
        high, rest = split(jnp.concatenate(sides, axis=0))
        terms = jnp.concatenate([high, rest], axis=0)
        again = jnp.concatenate([high, jnp.zeros_like(rest)], axis=0)
        terms = dot(jnp.concatenate([terms, again], axis=1), weights, 1, 0)
        coefficients = terms[: len(pair) * sketch_rows] + terms[len(pair) * sketch_rows :]
        for side, slot in pair:
            a, b = slots[slot]
            i, j = place(slot)
            c = coefficients[side * sketch_rows : (side + 1) * sketch_rows]
            c_out[a, 0, b, 0] = c
            gain = fold(c * (products[side] + shifts[side] * c))
            residuals[slot] = norms[slot] - jnp.where(j < i, gain, 0.0)

    def norm_wait(ref):
        return pltpu.make_async_remote_copy(
            src_ref=ref,
            dst_ref=ref,
            send_sem=sem_ns,
            recv_sem=sem_nr,
            device_id=(p, sibling),
            device_id_type=MESH,
        )

    others = norm_wait(sums.at[pl.ds(0, devices - 1)])
    others.wait_recv()
    whole_out[...] = jnp.sum(sums[...], axis=0)
    others.wait_send()

    for target in point_targets:
        pl.when(wants_points(q, target))(point_copy(q, target).wait_send)
    for other, wanted in bank_steps:
        pl.when(wanted)(bank_copy(q, other, sem_br.at[q]).wait_send)
    pl.when(beside)(bank_copy(0, sibling, sem_sr, cols // 2).wait_send)


def finish(rows, cols, row_tiles, col_tiles, y, c, residuals, whole, y_out, c_out, err_out, rank_out, sems):
    p = lax.axis_index("prow")
    q = lax.axis_index("pcol")
    copies = [
        pltpu.make_async_copy(source.at[a], target.at[a], sems.at[index, a])
        for index, (source, target) in enumerate([(y, y_out), (c, c_out)])
        for a in range(row_tiles)
    ]
    for copy in copies:
        copy.start()
    norm = lax.rsqrt(all_sum(whole[0:1, :])) * float(cols * col_tiles)
    lane = lax.broadcasted_iota(jnp.int32, (1, 128), 1)
    for b in range(col_tiles):
        line = jnp.zeros((1, 128), F32)
        for a in range(row_tiles):
            error = jnp.sqrt(jnp.maximum(all_sum(residuals[a * col_tiles + b]), 0.0)) * norm
            shown = (lane == a) & (b * cols + q <= a * rows + p)
            line = jnp.where(shown, error, line)
        err_out[0, b, 0:1, :] = line[:, :row_tiles]
    rank_out[0] = whole[1:2, 0:1].astype(jnp.int32)[0, 0]
    for copy in copies:
        copy.wait()


def per_device(rows, cols, points, range_length, smoothness, bank, ids, ranks):
    row_tiles, col_tiles = ids.shape[0], ids.shape[2]
    per_bank, sketch_rows, size = bank.shape
    slots = row_tiles * col_tiles
    ids = ids.transpose(1, 2, 3, 0)
    ranks = ranks.transpose(1, 2, 3, 0)
    factors = jax.ShapeDtypeStruct((row_tiles, 1, col_tiles, 1, sketch_rows, size), F32)
    vmem = pl.BlockSpec(memory_space=pltpu.VMEM)
    smem = pl.BlockSpec(memory_space=pltpu.SMEM)
    hbm = pl.BlockSpec(memory_space=pltpu.HBM)
    dma = pltpu.SemaphoreType.DMA
    pinned = [pltpu.with_memory_space_constraint(x, pltpu.HBM) for x in (points, bank, ids, ranks)]
    y, c, residuals, whole = pl.pallas_call(
        functools.partial(kernel, rows, cols, row_tiles, col_tiles),
        out_shape=(
            factors,
            factors,
            jax.ShapeDtypeStruct((slots, 8, 128), F32),
            jax.ShapeDtypeStruct((2, 128), F32),
        ),
        in_specs=[smem, smem, hbm, hbm, hbm, hbm],
        out_specs=(vmem,) * 4,
        scratch_shapes=[
            pltpu.SMEM(ids.shape, jnp.int32),
            pltpu.SMEM(ranks.shape, jnp.int32),
            pltpu.VMEM((cols, col_tiles, 2, size), F32),
            pltpu.VMEM((cols * per_bank, sketch_rows, size), BF16),
            pltpu.VMEM((slots, size, size), BF16),
            pltpu.VMEM((slots, 8, 128), F32),
            pltpu.VMEM((col_tiles, size, 128), F32),
            pltpu.VMEM((col_tiles, size, 128), F32),
            pltpu.VMEM((2, size), F32),
            pltpu.VMEM((2, 128), F32),
            pltpu.VMEM((rows * cols, 2, 128), F32),
            dma((4,)),
            dma,
            dma((cols,)),
            dma,
            dma((cols,)),
            dma,
            dma,
            dma,
            pltpu.SemaphoreType.REGULAR,
        ],
        compiler_params=pltpu.CompilerParams(
            collective_id=0, has_side_effects=True, vmem_limit_bytes=40 * 1024 * 1024
        ),
        name="tiles",
    )(range_length, smoothness, *pinned)
    y, c, errors, rank_total = pl.pallas_call(
        functools.partial(finish, rows, cols, row_tiles, col_tiles),
        out_shape=(
            factors,
            factors,
            jax.ShapeDtypeStruct((1, col_tiles, 1, row_tiles), F32),
            jax.ShapeDtypeStruct((1,), jnp.int32),
        ),
        in_specs=[vmem] * 4,
        out_specs=(hbm, hbm, vmem, smem),
        scratch_shapes=[dma((2, row_tiles))],
        compiler_params=pltpu.CompilerParams(vmem_limit_bytes=16 * 1024 * 1024),
        name="finish",
    )(y, c, residuals, whole)
    return y, c, errors.transpose(3, 0, 1, 2), rank_total


def solution(mesh):
    in_specs = (
        P(None, "pcol", None, None),
        P(),
        P(),
        P("pcol", None, None),
        P(None, "prow", None, "pcol"),
        P(None, "prow", None, "pcol"),
    )
    out_specs = (
        P(None, "prow", None, "pcol", None, None),
        P(None, "prow", None, "pcol", None, None),
        P(None, "prow", None, "pcol"),
        P(),
    )
    return jax.shard_map(
        functools.partial(per_device, mesh.shape["prow"], mesh.shape["pcol"]),
        mesh=mesh,
        in_specs=in_specs,
        out_specs=out_specs,
        check_vma=False,
    )
```

```python
import functools
import math

import jax
import jax.numpy as jnp
from jax import lax
from jax.experimental import pallas as pl
from jax.experimental.pallas import tpu as pltpu
from jax.sharding import PartitionSpec as P

MESH = pl.DeviceIdType.MESH
LOG2E = math.log2(math.e)
F32 = jnp.float32
BF16 = jnp.bfloat16
HIGH = lax.Precision.HIGHEST


def dot(a, b, da, db, precision=None):
    return lax.dot_general(
        a, b, (((da,), (db,)), ((), ())), preferred_element_type=F32, precision=precision
    )


def split(x):
    high = x.astype(BF16)
    return high, (x - high.astype(F32)).astype(BF16)


def all_sum(x):
    return jnp.sum(jnp.sum(x, axis=1, keepdims=True), axis=0, keepdims=True)


def invert(m, size, half, group=8):
    parts = size // 8
    width = m.shape[1]
    sub = lax.broadcasted_iota(jnp.int32, (8, width), 0)
    lane = lax.broadcasted_iota(jnp.int32, (8, width), 1)
    side = lane // half * half
    lane = lane - side
    m = [m[8 * v : 8 * v + 8] for v in range(parts)]
    for start in range(0, size, group):
        cols = {
            k: [jnp.take_along_axis(part, side + k, axis=1) for part in m]
            for k in range(start, start + group)
        }
        for k in range(start, start + group):
            at, within = divmod(k, 8)
            col = cols.pop(k)
            pivot = jnp.broadcast_to(col[at][within : within + 1], (8, width))
            inverse = 1.0 / pivot
            for other, entry in cols.items():
                head = jnp.broadcast_to(entry[at][within : within + 1], (8, width)) * inverse
                entry = [e - c * head for e, c in zip(entry, col)]
                entry[at] = jnp.where(sub == within, head, entry[at])
                cols[other] = entry
            row = jnp.broadcast_to(m[at][within : within + 1], (8, width))
            row = jnp.where(lane == k, 1.0, row) * inverse
            m = [jnp.where(lane == k, 0.0, part) - c * row for part, c in zip(m, col)]
            m[at] = jnp.where(sub == within, row, m[at])
    return jnp.concatenate(m, axis=0)


def fold(x):
    rows, width = x.shape
    x = jnp.sum(x.reshape(rows // 8, 8, width), axis=0)
    return functools.reduce(jnp.add, [x[:, n : n + 128] for n in range(0, width, 128)])


def kernel(
    rows,
    cols,
    row_tiles,
    col_tiles,
    range_length,
    smoothness,
    points_hbm,
    bank_hbm,
    ids_hbm,
    ranks_hbm,
    y_out,
    c_out,
    residuals,
    whole_out,
    ids,
    ranks,
    all_points,
    all_bank,
    low,
    norms,
    x_spread,
    y_spread,
    line,
    mine,
    sums,
    sem_local,
    sem_ps,
    sem_pr,
    sem_bs,
    sem_br,
    sem_sr,
    sem_ns,
    sem_nr,
    ready,
):
    p = lax.axis_index("prow")
    q = lax.axis_index("pcol")
    per_bank, sketch_rows, size = bank_hbm.shape
    slots = [(a, b) for a in range(row_tiles) for b in range(col_tiles)]
    sibling = q + 1 - 2 * lax.rem(q, 2)
    mirrored = row_tiles == 2 and col_tiles == 1 and cols == 2 * rows

    barrier = pltpu.get_barrier_semaphore()
    for step in range(1, cols):
        pl.semaphore_signal(
            barrier, device_id=(p, lax.rem(q + step, cols)), device_id_type=MESH
        )
    gate = q == 0

    def tell_gates(semaphore):
        for step in range(1, rows):
            pl.semaphore_signal(
                semaphore, device_id=(lax.rem(p + step, rows), 0), device_id_type=MESH
            )

    @pl.when(gate)
    def _():
        tell_gates(barrier)

    own_bank = pl.ds(q * per_bank, per_bank)
    local = [
        pltpu.make_async_copy(source, target, sem_local.at[index])
        for index, (source, target) in enumerate(
            [
                (points_hbm.at[:, 0], all_points.at[q]),
                (bank_hbm, all_bank.at[own_bank]),
                (ids_hbm, ids),
                (ranks_hbm, ranks),
            ]
        )
    ]
    for copy in local:
        copy.start()
    def place(slot):
        a, b = slots[slot]
        return a * rows + p, b * cols + q

    def wants_bank(device):
        wanted = device < 0
        for a, b in slots:
            wanted = wanted | (b * cols + device < a * rows + p)
        return wanted

    def wants_points(source, target):
        if mirrored:
            early = (source == p) & ((target < p) | (target >= p + rows))
            return early | ((source == p + rows) & (target < source))
        wanted = source < 0
        for a in range(row_tiles):
            wanted = wanted | (lax.rem(a * rows + p, cols) == source)
        return wanted

    bank_steps = []
    for step in sorted(range(2, cols, 2), key=lambda step: step == cols // 2):
        other = lax.rem(q + step, cols)
        twin = other + 1 - 2 * lax.rem(other, 2)
        bank_steps.append((other, wants_bank(other) | wants_bank(twin)))
    here, beside = wants_bank(q), wants_bank(sibling)

    def clear(slot):
        norms[slot] = jnp.zeros((8, 128), F32)

        def chunk(c, _):
            low[slot, pl.ds(pl.multiple_of(c * 128, 128), 128)] = jnp.zeros((128, size), BF16)
            return 0

        lax.fori_loop(0, size // 128, chunk, 0)

    for slot in range(len(slots)):
        i, j = place(slot)
        pl.when(j > i)(functools.partial(clear, slot))

        @pl.when(j >= i)
        def _():
            a, b = slots[slot]
            y_out[a, 0, b, 0] = jnp.zeros((sketch_rows, size), F32)
    for copy in local:
        copy.wait()

    def point_copy(source, target):
        return pltpu.make_async_remote_copy(
            src_ref=all_points.at[source],
            dst_ref=all_points.at[source],
            send_sem=sem_ps,
            recv_sem=sem_pr.at[source],
            device_id=(p, target),
            device_id_type=MESH,
        )

    def bank_copy(block, target, recv, count=1):
        at = pl.ds(block * per_bank, per_bank * count)
        return pltpu.make_async_remote_copy(
            src_ref=all_bank.at[at],
            dst_ref=all_bank.at[at],
            send_sem=sem_bs,
            recv_sem=recv,
            device_id=(p, target),
            device_id_type=MESH,
        )

    degree = jnp.full((8, 128), smoothness[0].astype(F32))
    scale = (LOG2E * jnp.sqrt(2.0 * degree + 1.0)) / jnp.full((8, 128), range_length[0])
    scale = scale[:1]
    linear, square = 1.0 / LOG2E, 1.0 / (3.0 * LOG2E * LOG2E)

    def by_order(zero, one, two):
        return jnp.where(smoothness[0] >= 2, two, jnp.where(smoothness[0] >= 1, one, zero)).astype(F32)

    offset = by_order(-38.0, -31.0, math.log2(square))
    first = by_order(0.0, linear * 2.0**31, linear / square)
    constant = by_order(2.0**38, 2.0**31, 1.0 / square)
    for b in range(col_tiles):
        for n in range(0, size, 128):
            cut = slice(n, n + 128)
            x_own = all_points[q, b, 0:1, cut] * scale
            y_own = all_points[q, b, 1:2, cut] * scale
            x_spread[b, cut] = jnp.broadcast_to(x_own, (128, 128)).T
            y_spread[b, cut] = jnp.broadcast_to(y_own, (128, 128)).T

    def generate(slot, begin=0, end=size // 128):
        i, j = place(slot)
        b = slots[slot][1]
        row_block, row_major = lax.rem(i, cols), i // cols
        for n in range(0, size, 128):
            cut = slice(n, n + 128)
            line[:, cut] = all_points[row_block, row_major, :, cut] * scale

        def chunk(c, total):
            at = pl.ds(pl.multiple_of(c * 128, 128), 128)
            x_own, y_own = x_spread[b, at], y_spread[b, at]
            for n in range(0, size, 128):
                cut = slice(n, n + 128)
                dx = x_own - line[0:1, cut]
                dy = y_own - line[1:2, cut]
                d2 = dx * dx + dy * dy
                t = d2 * lax.rsqrt(jnp.maximum(d2, 1e-30))
                tile = ((constant + t * (first + t)) * jnp.exp2(offset - t)).astype(BF16)
                low[slot, at, cut] = tile
                tile = tile.astype(F32)
                total = total + jnp.sum((tile * tile).reshape(16, 8, 128), axis=0)
            return total

        total = jnp.zeros((8, 128), F32) if begin == 0 else norms[slot]
        norms[slot] = lax.fori_loop(begin, end, chunk, total)

    i, j = place(0)
    pl.when((i == 0) & (j == 0))(functools.partial(generate, 0))

    pl.semaphore_wait(barrier, cols - 1 + jnp.where(gate, rows - 1, 0))

    point_targets = [lax.rem(q + cols - step, cols) for step in range(1, cols)]
    for target in point_targets:
        pl.when(wants_points(q, target))(point_copy(q, target).start)
    for other, wanted in bank_steps[:-1]:
        pl.when(wanted)(bank_copy(q, other, sem_br.at[q]).start)
    for other, wanted in bank_steps[-1:]:
        pl.when(wanted)(bank_copy(q, other, sem_br.at[q]).start)
    pl.when(beside)(bank_copy(q, sibling, sem_sr).start)
    @pl.when(gate)
    def _():
        tell_gates(ready)

    def open_gate():
        pl.semaphore_wait(ready, rows - 1)
        for step in range(1, cols):
            pl.semaphore_signal(ready, device_id=(p, step), device_id_type=MESH)


    def forward():
        for other, _ in bank_steps:
            pl.when(here | beside)(bank_copy(other, q, sem_br.at[other]).wait_recv)
            pl.when(beside)(bank_copy(other, sibling, sem_sr).start)

    devices = rows * cols
    me = p * cols + q

    def norm_copy(target):
        return pltpu.make_async_remote_copy(
            src_ref=mine,
            dst_ref=sums.at[me],
            send_sem=sem_ns,
            recv_sem=sem_nr,
            device_id=(target // cols, lax.rem(target, cols)),
            device_id_type=MESH,
        )

    def send_norms(weights):
        norm_sum = jnp.zeros((8, 128), F32)
        rank_sum = jnp.float32(0)
        for slot, (a, b) in enumerate(slots):
            i, j = place(slot)
            norm_sum = norm_sum + weights[slot] * norms[slot]
            rank_sum = rank_sum + jnp.where(j < i, ranks[0, b, 0, a], 0).astype(F32)
        mine[0:1, :] = jnp.sum(norm_sum, axis=0, keepdims=True)
        mine[1:2, :] = jnp.full((1, 128), rank_sum)
        sums[me] = mine[...]
        pl.when(~gate)(functools.partial(pl.semaphore_wait, ready, 1))
        for step in range(1, devices):
            norm_copy(lax.rem(me + step, devices)).start()

    arrived = []

    def await_points(a):
        owner = lax.rem(a * rows + p, cols)
        fresh = owner != q
        for before in arrived:
            fresh = fresh & (owner != lax.rem(before * rows + p, cols))
        arrived.append(a)

        @pl.when(fresh & wants_points(owner, q))
        def _():
            point_copy(owner, q).wait_recv()

    if mirrored:
        middle = size // 256
        both, lone = q <= p, (q > p) & (q <= p + rows)
        pl.when(q == p + rows)(functools.partial(generate, 1))
        await_points(0)
        pl.when(gate & (p > 0))(functools.partial(generate, 0, 0, middle))
        pl.when(gate)(open_gate)
        pl.when(gate & (p > 0))(functools.partial(generate, 0, middle))
        pl.when((both & ~gate) | (q >= p + rows))(functools.partial(generate, 0))
        await_points(1)
        alone = lone & (q < p + rows)
        early = alone & (sibling == p)
        late = size * 3 // 512
        pl.when(alone)(functools.partial(generate, 1, 0, late))
        pl.when(early)(forward)
        pl.when(alone)(functools.partial(generate, 1, late))
        from_first = jnp.where((q < p) | (q >= p + rows), 2.0, jnp.where(q == p, 1.0, 0.0))
        from_second = jnp.where(lone, jnp.where(q < p + rows, 2.0, 1.0), 0.0)
        send_norms([from_first, from_second])
        pl.when(both)(functools.partial(generate, 1, 0, middle))
        pl.when(~early)(forward)
        pl.when(both)(functools.partial(generate, 1, middle))
    else:
        for slot, (a, b) in enumerate(slots):
            i, j = place(slot)
            if a not in arrived:
                await_points(a)
            pl.when((j <= i) & (i + j > 0) if slot == 0 else j <= i)(functools.partial(generate, slot))
        pl.when(gate)(open_gate)
        weights = []
        for slot in range(len(slots)):
            i, j = place(slot)
            weights.append(jnp.where(j < i, 2.0, 1.0))
        send_norms(weights)
        forward()

    pl.when(here)(bank_copy(0, q, sem_sr, cols // 2).wait_recv)

    half = 64
    row_at = lax.broadcasted_iota(jnp.int32, (sketch_rows, 1), 0)

    def rank_of(slot):
        a, b = slots[slot]
        i, j = place(slot)
        return jnp.where(j < i, ranks[0, b, 0, a], 0)

    def valid(slot):
        i, j = place(slot)
        return j < i

    def sketch_tile(slot):
        a, b = slots[slot]
        sketch = all_bank[ids[0, b, 0, a]]
        sketch = jnp.where(row_at < ranks[0, b, 0, a], sketch.astype(F32), 0.0).astype(BF16)
        y_out[a, 0, b, 0] = dot(sketch, low[slot], 1, 0)

    blank = jnp.zeros((half - sketch_rows, size), BF16)

    def stack(parts):
        full = [x for part in parts for x in (part, blank)]
        if len(parts) == 1:
            full += full[:1] + [blank]
        return jnp.concatenate(full, axis=0)

    for first in range(0, len(slots), 2):
        pair = list(enumerate(range(first, min(first + 2, len(slots)))))
        highs, lows = [], []
        for side, slot in pair:
            pl.when(valid(slot))(functools.partial(sketch_tile, slot))
        for side, slot in pair:
            a, b = slots[slot]
            high, rest = split(y_out[a, 0, b, 0])
            highs.append(high)
            lows.append(rest)
        high, rest = stack(highs), stack(lows)
        gram = dot(jnp.concatenate([high, rest], axis=0), high, 1, 1)
        gram = gram[: 2 * half] + gram[2 * half :] + dot(high, rest, 1, 1)
        lane = lax.broadcasted_iota(jnp.int32, (sketch_rows, 2 * half), 1)
        sub = lax.broadcasted_iota(jnp.int32, (sketch_rows, 2 * half), 0)
        left = lane < half
        gram = jnp.where(left, gram[:sketch_rows], gram[half : half + sketch_rows])
        eye = lane == jnp.where(left, sub, sub + half)
        shifts = []
        diagonal = jnp.ones((sketch_rows, 2 * half), F32)
        for side, slot in pair:
            a, b = slots[slot]
            mask = left if side == 0 else ~left
            rank = jnp.full((1, 1), ranks[0, b, 0, a].astype(F32))
            shift = 0.1 * all_sum(jnp.where(eye & mask, gram, 0.0)) / rank
            shifts.append(shift)
            diagonal = jnp.where(mask & (sub < rank_of(slot)), shift, diagonal)
        inverse = invert(gram + jnp.where(eye, diagonal, 0.0), sketch_rows, half)
        products, highs_w, lows_w = [], [], []
        for side, slot in pair:
            product = dot(jnp.concatenate([highs[side], lows[side]], axis=0), low[slot], 1, 1)
            high, rest = split(product[:sketch_rows])
            highs_w.append(high)
            lows_w.append(rest)
            products.append(product[:sketch_rows] + 2.0 * product[sketch_rows:])
        weights = jnp.concatenate([stack(highs_w), stack(lows_w)], axis=0)
        sides = [jnp.where(left if side == 0 else ~left, inverse, 0.0) for side, _ in pair]
        high, rest = split(jnp.concatenate(sides, axis=0))
        terms = jnp.concatenate([high, rest], axis=0)
        again = jnp.concatenate([high, jnp.zeros_like(rest)], axis=0)
        terms = dot(jnp.concatenate([terms, again], axis=1), weights, 1, 0)
        coefficients = terms[: len(pair) * sketch_rows] + terms[len(pair) * sketch_rows :]
        for side, slot in pair:
            a, b = slots[slot]
            i, j = place(slot)
            c = coefficients[side * sketch_rows : (side + 1) * sketch_rows]
            c_out[a, 0, b, 0] = c
            gain = fold(c * (products[side] + shifts[side] * c))
            residuals[slot] = norms[slot] - jnp.where(j < i, gain, 0.0)

    def norm_wait(ref):
        return pltpu.make_async_remote_copy(
            src_ref=ref,
            dst_ref=ref,
            send_sem=sem_ns,
            recv_sem=sem_nr,
            device_id=(p, sibling),
            device_id_type=MESH,
        )

    others = norm_wait(sums.at[pl.ds(0, devices - 1)])
    others.wait_recv()
    whole_out[...] = jnp.sum(sums[...], axis=0)
    others.wait_send()

    owns_points = q < 0
    for a in range(row_tiles):
        owns_points = owns_points | (lax.rem(a * rows + p, cols) == q)

    @pl.when(owns_points)
    def _():
        for target in point_targets:
            pl.when(wants_points(q, target))(point_copy(q, target).wait_send)

    for other, wanted in bank_steps:
        pl.when(wanted)(bank_copy(q, other, sem_br.at[q]).wait_send)
    pl.when(beside)(bank_copy(0, sibling, sem_sr, cols // 2).wait_send)


def finish(rows, cols, row_tiles, col_tiles, y, c, residuals, whole, y_out, c_out, err_out, rank_out, sems):
    p = lax.axis_index("prow")
    q = lax.axis_index("pcol")
    copies = [
        pltpu.make_async_copy(source.at[a], target.at[a], sems.at[index, a])
        for index, (source, target) in enumerate([(y, y_out), (c, c_out)])
        for a in range(row_tiles)
    ]
    for copy in copies:
        copy.start()
    norm = lax.rsqrt(all_sum(whole[0:1, :])) * float(cols * col_tiles)
    lane = lax.broadcasted_iota(jnp.int32, (1, 128), 1)
    for b in range(col_tiles):
        line = jnp.zeros((1, 128), F32)
        for a in range(row_tiles):
            error = jnp.sqrt(jnp.maximum(all_sum(residuals[a * col_tiles + b]), 0.0)) * norm
            shown = (lane == a) & (b * cols + q <= a * rows + p)
            line = jnp.where(shown, error, line)
        err_out[0, b, 0:1, :] = line[:, :row_tiles]
    rank_out[0] = whole[1:2, 0:1].astype(jnp.int32)[0, 0]
    for copy in copies:
        copy.wait()


def per_device(rows, cols, points, range_length, smoothness, bank, ids, ranks):
    row_tiles, col_tiles = ids.shape[0], ids.shape[2]
    per_bank, sketch_rows, size = bank.shape
    slots = row_tiles * col_tiles
    ids = ids.transpose(1, 2, 3, 0)
    ranks = ranks.transpose(1, 2, 3, 0)
    factors = jax.ShapeDtypeStruct((row_tiles, 1, col_tiles, 1, sketch_rows, size), F32)
    vmem = pl.BlockSpec(memory_space=pltpu.VMEM)
    smem = pl.BlockSpec(memory_space=pltpu.SMEM)
    hbm = pl.BlockSpec(memory_space=pltpu.HBM)
    dma = pltpu.SemaphoreType.DMA
    pinned = [pltpu.with_memory_space_constraint(x, pltpu.HBM) for x in (points, bank, ids, ranks)]
    y, c, residuals, whole = pl.pallas_call(
        functools.partial(kernel, rows, cols, row_tiles, col_tiles),
        out_shape=(
            factors,
            factors,
            jax.ShapeDtypeStruct((slots, 8, 128), F32),
            jax.ShapeDtypeStruct((2, 128), F32),
        ),
        in_specs=[smem, smem, hbm, hbm, hbm, hbm],
        out_specs=(vmem,) * 4,
        scratch_shapes=[
            pltpu.SMEM(ids.shape, jnp.int32),
            pltpu.SMEM(ranks.shape, jnp.int32),
            pltpu.VMEM((cols, col_tiles, 2, size), F32),
            pltpu.VMEM((cols * per_bank, sketch_rows, size), BF16),
            pltpu.VMEM((slots, size, size), BF16),
            pltpu.VMEM((slots, 8, 128), F32),
            pltpu.VMEM((col_tiles, size, 128), F32),
            pltpu.VMEM((col_tiles, size, 128), F32),
            pltpu.VMEM((2, size), F32),
            pltpu.VMEM((2, 128), F32),
            pltpu.VMEM((rows * cols, 2, 128), F32),
            dma((4,)),
            dma,
            dma((cols,)),
            dma,
            dma((cols,)),
            dma,
            dma,
            dma,
            pltpu.SemaphoreType.REGULAR,
        ],
        compiler_params=pltpu.CompilerParams(
            collective_id=0, has_side_effects=True, vmem_limit_bytes=40 * 1024 * 1024
        ),
        name="tiles",
    )(range_length, smoothness, *pinned)
    y, c, errors, rank_total = pl.pallas_call(
        functools.partial(finish, rows, cols, row_tiles, col_tiles),
        out_shape=(
            factors,
            factors,
            jax.ShapeDtypeStruct((1, col_tiles, 1, row_tiles), F32),
            jax.ShapeDtypeStruct((1,), jnp.int32),
        ),
        in_specs=[vmem] * 4,
        out_specs=(hbm, hbm, vmem, smem),
        scratch_shapes=[dma((2, row_tiles))],
        compiler_params=pltpu.CompilerParams(vmem_limit_bytes=16 * 1024 * 1024),
        name="finish",
    )(y, c, residuals, whole)
    return y, c, errors.transpose(3, 0, 1, 2), rank_total


def solution(mesh):
    in_specs = (
        P(None, "pcol", None, None),
        P(),
        P(),
        P("pcol", None, None),
        P(None, "prow", None, "pcol"),
        P(None, "prow", None, "pcol"),
    )
    out_specs = (
        P(None, "prow", None, "pcol", None, None),
        P(None, "prow", None, "pcol", None, None),
        P(None, "prow", None, "pcol"),
        P(),
    )
    return jax.shard_map(
        functools.partial(per_device, mesh.shape["prow"], mesh.shape["pcol"]),
        mesh=mesh,
        in_specs=in_specs,
        out_specs=out_specs,
        check_vma=False,
    )
```

```python
import functools
import math

import jax
import jax.numpy as jnp
from jax import lax
from jax.experimental import pallas as pl
from jax.experimental.pallas import tpu as pltpu
from jax.sharding import PartitionSpec as P

MESH = pl.DeviceIdType.MESH
LOG2E = math.log2(math.e)
F32 = jnp.float32
BF16 = jnp.bfloat16
HIGH = lax.Precision.HIGHEST


def dot(a, b, da, db, precision=None):
    return lax.dot_general(
        a, b, (((da,), (db,)), ((), ())), preferred_element_type=F32, precision=precision
    )


def split(x):
    high = x.astype(BF16)
    return high, (x - high.astype(F32)).astype(BF16)


def all_sum(x):
    return jnp.sum(jnp.sum(x, axis=1, keepdims=True), axis=0, keepdims=True)


def invert(m, size, half, group=8):
    parts = size // 8
    width = m.shape[1]
    sub = lax.broadcasted_iota(jnp.int32, (8, width), 0)
    lane = lax.broadcasted_iota(jnp.int32, (8, width), 1)
    side = lane // half * half
    lane = lane - side
    m = [m[8 * v : 8 * v + 8] for v in range(parts)]
    for start in range(0, size, group):
        cols = {
            k: [jnp.take_along_axis(part, side + k, axis=1) for part in m]
            for k in range(start, start + group)
        }
        for k in range(start, start + group):
            at, within = divmod(k, 8)
            col = cols.pop(k)
            pivot = jnp.broadcast_to(col[at][within : within + 1], (8, width))
            inverse = 1.0 / pivot
            for other, entry in cols.items():
                head = jnp.broadcast_to(entry[at][within : within + 1], (8, width)) * inverse
                entry = [e - c * head for e, c in zip(entry, col)]
                entry[at] = jnp.where(sub == within, head, entry[at])
                cols[other] = entry
            row = jnp.broadcast_to(m[at][within : within + 1], (8, width))
            row = jnp.where(lane == k, 1.0, row) * inverse
            m = [jnp.where(lane == k, 0.0, part) - c * row for part, c in zip(m, col)]
            m[at] = jnp.where(sub == within, row, m[at])
    return jnp.concatenate(m, axis=0)


def fold(x):
    rows, width = x.shape
    x = jnp.sum(x.reshape(rows // 8, 8, width), axis=0)
    return functools.reduce(jnp.add, [x[:, n : n + 128] for n in range(0, width, 128)])


def kernel(
    rows,
    cols,
    row_tiles,
    col_tiles,
    range_length,
    smoothness,
    points_hbm,
    bank_hbm,
    ids_hbm,
    ranks_hbm,
    y_out,
    c_out,
    residuals,
    whole_out,
    ids,
    ranks,
    all_points,
    all_bank,
    low,
    norms,
    x_spread,
    y_spread,
    line,
    mine,
    sums,
    sem_local,
    sem_ps,
    sem_pr,
    sem_bs,
    sem_br,
    sem_sr,
    sem_ns,
    sem_nr,
    ready,
):
    p = lax.axis_index("prow")
    q = lax.axis_index("pcol")
    per_bank, sketch_rows, size = bank_hbm.shape
    slots = [(a, b) for a in range(row_tiles) for b in range(col_tiles)]
    sibling = q + 1 - 2 * lax.rem(q, 2)
    mirrored = row_tiles == 2 and col_tiles == 1 and cols == 2 * rows

    barrier = pltpu.get_barrier_semaphore()
    for step in range(1, cols):
        pl.semaphore_signal(
            barrier, device_id=(p, lax.rem(q + step, cols)), device_id_type=MESH
        )
    gate = q == 0

    def tell_gates(semaphore):
        for step in range(1, rows):
            pl.semaphore_signal(
                semaphore, device_id=(lax.rem(p + step, rows), 0), device_id_type=MESH
            )

    @pl.when(gate)
    def _():
        tell_gates(barrier)

    own_bank = pl.ds(q * per_bank, per_bank)
    local = [
        pltpu.make_async_copy(source, target, sem_local.at[index])
        for index, (source, target) in enumerate(
            [
                (points_hbm.at[:, 0], all_points.at[q]),
                (bank_hbm, all_bank.at[own_bank]),
                (ids_hbm, ids),
                (ranks_hbm, ranks),
            ]
        )
    ]
    for copy in local:
        copy.start()
    def place(slot):
        a, b = slots[slot]
        return a * rows + p, b * cols + q

    def wants_bank(device):
        wanted = device < 0
        for a, b in slots:
            wanted = wanted | (b * cols + device < a * rows + p)
        return wanted

    def wants_points(source, target):
        if mirrored:
            early = (source == p) & ((target < p) | (target >= p + rows))
            return early | ((source == p + rows) & (target < source))
        wanted = source < 0
        for a in range(row_tiles):
            wanted = wanted | (lax.rem(a * rows + p, cols) == source)
        return wanted

    bank_steps = []
    turned = q + 2 - 4 * lax.rem(q // 2, 2)
    nearest = [turned] + [lax.rem(q + step, cols) for step in range(4, cols, 4)]
    farther = [lax.rem(turned + step, cols) for step in range(4, cols, 4)]
    for other in nearest + farther:
        twin = other + 1 - 2 * lax.rem(other, 2)
        bank_steps.append((other, wants_bank(other) | wants_bank(twin)))
    here, beside = wants_bank(q), wants_bank(sibling)

    def clear(slot):
        norms[slot] = jnp.zeros((8, 128), F32)

        def chunk(c, _):
            low[slot, pl.ds(pl.multiple_of(c * 128, 128), 128)] = jnp.zeros((128, size), BF16)
            return 0

        lax.fori_loop(0, size // 128, chunk, 0)

    for slot in range(len(slots)):
        i, j = place(slot)
        pl.when(j > i)(functools.partial(clear, slot))

        @pl.when(j >= i)
        def _():
            a, b = slots[slot]
            y_out[a, 0, b, 0] = jnp.zeros((sketch_rows, size), F32)
    for copy in local:
        copy.wait()

    def point_copy(source, target):
        return pltpu.make_async_remote_copy(
            src_ref=all_points.at[source],
            dst_ref=all_points.at[source],
            send_sem=sem_ps,
            recv_sem=sem_pr.at[source],
            device_id=(p, target),
            device_id_type=MESH,
        )

    def bank_copy(block, target, recv, count=1):
        at = pl.ds(block * per_bank, per_bank * count)
        return pltpu.make_async_remote_copy(
            src_ref=all_bank.at[at],
            dst_ref=all_bank.at[at],
            send_sem=sem_bs,
            recv_sem=recv,
            device_id=(p, target),
            device_id_type=MESH,
        )

    degree = jnp.full((8, 128), smoothness[0].astype(F32))
    scale = (LOG2E * jnp.sqrt(2.0 * degree + 1.0)) / jnp.full((8, 128), range_length[0])
    scale = scale[:1]
    linear, square = 1.0 / LOG2E, 1.0 / (3.0 * LOG2E * LOG2E)

    def by_order(zero, one, two):
        return jnp.where(smoothness[0] >= 2, two, jnp.where(smoothness[0] >= 1, one, zero)).astype(F32)

    offset = by_order(-38.0, -31.0, math.log2(square))
    first = by_order(0.0, linear * 2.0**31, linear / square)
    constant = by_order(2.0**38, 2.0**31, 1.0 / square)
    for b in range(col_tiles):
        for n in range(0, size, 128):
            cut = slice(n, n + 128)
            x_own = all_points[q, b, 0:1, cut] * scale
            y_own = all_points[q, b, 1:2, cut] * scale
            x_spread[b, cut] = jnp.broadcast_to(x_own, (128, 128)).T
            y_spread[b, cut] = jnp.broadcast_to(y_own, (128, 128)).T

    def generate(slot, begin=0, end=size // 128):
        i, j = place(slot)
        b = slots[slot][1]
        row_block, row_major = lax.rem(i, cols), i // cols
        for n in range(0, size, 128):
            cut = slice(n, n + 128)
            line[:, cut] = all_points[row_block, row_major, :, cut] * scale

        def chunk(c, total):
            at = pl.ds(pl.multiple_of(c * 128, 128), 128)
            x_own, y_own = x_spread[b, at], y_spread[b, at]
            for n in range(0, size, 128):
                cut = slice(n, n + 128)
                dx = x_own - line[0:1, cut]
                dy = y_own - line[1:2, cut]
                d2 = dx * dx + dy * dy
                t = d2 * lax.rsqrt(jnp.maximum(d2, 1e-30))
                tile = ((constant + t * (first + t)) * jnp.exp2(offset - t)).astype(BF16)
                low[slot, at, cut] = tile
                tile = tile.astype(F32)
                total = total + jnp.sum((tile * tile).reshape(16, 8, 128), axis=0)
            return total

        total = jnp.zeros((8, 128), F32) if begin == 0 else norms[slot]
        norms[slot] = lax.fori_loop(begin, end, chunk, total)

    i, j = place(0)
    pl.when((i == 0) & (j == 0))(functools.partial(generate, 0))

    pl.semaphore_wait(barrier, cols - 1 + jnp.where(gate, rows - 1, 0))

    point_targets = [lax.rem(q + cols - step, cols) for step in range(1, cols)]
    for target in point_targets:
        pl.when(wants_points(q, target))(point_copy(q, target).start)
    for other, wanted in bank_steps[: len(nearest)]:
        pl.when(wanted)(bank_copy(q, other, sem_br.at[q]).start)
    pl.when((q != p) & (q != p + rows))(lambda: pl.delay(800))
    for other, wanted in bank_steps[len(nearest) :]:
        pl.when(wanted)(bank_copy(q, other, sem_br.at[q]).start)
    pl.when(beside)(bank_copy(q, sibling, sem_sr).start)
    @pl.when(gate)
    def _():
        tell_gates(ready)

    def open_gate():
        pl.semaphore_wait(ready, rows - 1)
        for step in range(1, cols):
            pl.semaphore_signal(ready, device_id=(p, step), device_id_type=MESH)


    def forward():
        for other, _ in bank_steps:
            pl.when(here | beside)(bank_copy(other, q, sem_br.at[other]).wait_recv)
            pl.when(beside)(bank_copy(other, sibling, sem_sr).start)

    devices = rows * cols
    me = p * cols + q

    def norm_copy(target):
        return pltpu.make_async_remote_copy(
            src_ref=mine,
            dst_ref=sums.at[me],
            send_sem=sem_ns,
            recv_sem=sem_nr,
            device_id=(target // cols, lax.rem(target, cols)),
            device_id_type=MESH,
        )

    def send_norms(weights):
        norm_sum = jnp.zeros((8, 128), F32)
        rank_sum = jnp.float32(0)
        for slot, (a, b) in enumerate(slots):
            i, j = place(slot)
            norm_sum = norm_sum + weights[slot] * norms[slot]
            rank_sum = rank_sum + jnp.where(j < i, ranks[0, b, 0, a], 0).astype(F32)
        mine[0:1, :] = jnp.sum(norm_sum, axis=0, keepdims=True)
        mine[1:2, :] = jnp.full((1, 128), rank_sum)
        sums[me] = mine[...]
        pl.when(~gate)(functools.partial(pl.semaphore_wait, ready, 1))
        for step in range(1, devices):
            norm_copy(lax.rem(me + step, devices)).start()

    arrived = []

    def await_points(a, skip=None):
        owner = lax.rem(a * rows + p, cols)
        fresh = owner != q
        for before in arrived:
            fresh = fresh & (owner != lax.rem(before * rows + p, cols))
        arrived.append(a)

        fresh = fresh & wants_points(owner, q)

        @pl.when(fresh if skip is None else fresh & ~skip)
        def _():
            point_copy(owner, q).wait_recv()

    if mirrored:
        middle = size // 256
        both, lone = q <= p, (q > p) & (q <= p + rows)
        pl.when(q == p + rows)(functools.partial(generate, 1))
        await_points(0)
        corner = gate & (p == 0)
        pl.when(corner)(point_copy(rows, q).wait_recv)
        pl.when(corner)(functools.partial(generate, 1, 0, middle))
        pl.when(gate & (p > 0))(functools.partial(generate, 0, 0, middle))
        pl.when(gate)(open_gate)
        pl.when(gate & (p > 0))(functools.partial(generate, 0, middle))
        pl.when((both & ~gate) | (q >= p + rows))(functools.partial(generate, 0))
        await_points(1, corner)
        alone = lone & (q < p + rows)
        early = alone & (sibling == p)
        late = size * 3 // 512
        pl.when(alone)(functools.partial(generate, 1, 0, late))
        pl.when(early)(forward)
        pl.when(alone)(functools.partial(generate, 1, late))
        from_first = jnp.where((q < p) | (q >= p + rows), 2.0, jnp.where(q == p, 1.0, 0.0))
        from_second = jnp.where(lone, jnp.where(q < p + rows, 2.0, 1.0), 0.0)
        send_norms([from_first, from_second])
        pl.when(both & ~corner)(functools.partial(generate, 1, 0, middle))
        pl.when(~early)(forward)
        pl.when(both)(functools.partial(generate, 1, middle))
    else:
        for slot, (a, b) in enumerate(slots):
            i, j = place(slot)
            if a not in arrived:
                await_points(a)
            pl.when((j <= i) & (i + j > 0) if slot == 0 else j <= i)(functools.partial(generate, slot))
        pl.when(gate)(open_gate)
        weights = []
        for slot in range(len(slots)):
            i, j = place(slot)
            weights.append(jnp.where(j < i, 2.0, 1.0))
        send_norms(weights)
        forward()

    pl.when(here)(bank_copy(0, q, sem_sr, cols // 2).wait_recv)

    half = 64
    row_at = lax.broadcasted_iota(jnp.int32, (sketch_rows, 1), 0)

    def rank_of(slot):
        a, b = slots[slot]
        i, j = place(slot)
        return jnp.where(j < i, ranks[0, b, 0, a], 0)

    def valid(slot):
        i, j = place(slot)
        return j < i

    def sketch_tile(slot):
        a, b = slots[slot]
        sketch = all_bank[ids[0, b, 0, a]]
        sketch = jnp.where(row_at < ranks[0, b, 0, a], sketch.astype(F32), 0.0).astype(BF16)
        y_out[a, 0, b, 0] = dot(sketch, low[slot], 1, 0)

    blank = jnp.zeros((half - sketch_rows, size), BF16)

    def stack(parts):
        full = [x for part in parts for x in (part, blank)]
        if len(parts) == 1:
            full += full[:1] + [blank]
        return jnp.concatenate(full, axis=0)

    for first in range(0, len(slots), 2):
        pair = list(enumerate(range(first, min(first + 2, len(slots)))))
        highs, lows = [], []
        wanted = [valid(slot) for _, slot in pair]
        every = functools.reduce(jnp.logical_and, wanted)

        @pl.when(every)
        def _():
            for _, slot in pair:
                sketch_tile(slot)

        for (_, slot), want in zip(pair, wanted):
            pl.when(want & ~every)(functools.partial(sketch_tile, slot))

        for side, slot in pair:
            a, b = slots[slot]
            high, rest = split(y_out[a, 0, b, 0])
            highs.append(high)
            lows.append(rest)
        high, rest = stack(highs), stack(lows)
        gram = dot(jnp.concatenate([high, rest], axis=0), high, 1, 1)
        gram = gram[: 2 * half] + gram[2 * half :] + dot(high, rest, 1, 1)
        lane = lax.broadcasted_iota(jnp.int32, (sketch_rows, 2 * half), 1)
        sub = lax.broadcasted_iota(jnp.int32, (sketch_rows, 2 * half), 0)
        left = lane < half
        gram = jnp.where(left, gram[:sketch_rows], gram[half : half + sketch_rows])
        eye = lane == jnp.where(left, sub, sub + half)
        shifts = []
        diagonal = jnp.ones((sketch_rows, 2 * half), F32)
        for side, slot in pair:
            a, b = slots[slot]
            mask = left if side == 0 else ~left
            rank = jnp.full((1, 1), ranks[0, b, 0, a].astype(F32))
            shift = 0.1 * all_sum(jnp.where(eye & mask, gram, 0.0)) / rank
            shifts.append(shift)
            diagonal = jnp.where(mask & (sub < rank_of(slot)), shift, diagonal)
        inverse = invert(gram + jnp.where(eye, diagonal, 0.0), sketch_rows, half)
        products, highs_w, lows_w = [], [], []
        for side, slot in pair:
            product = dot(jnp.concatenate([highs[side], lows[side]], axis=0), low[slot], 1, 1)
            high, rest = split(product[:sketch_rows])
            highs_w.append(high)
            lows_w.append(rest)
            products.append(product[:sketch_rows] + 2.0 * product[sketch_rows:])
        weights = jnp.concatenate([stack(highs_w), stack(lows_w)], axis=0)
        sides = [jnp.where(left if side == 0 else ~left, inverse, 0.0) for side, _ in pair]
        high, rest = split(jnp.concatenate(sides, axis=0))
        terms = jnp.concatenate([high, rest], axis=0)
        again = jnp.concatenate([high, jnp.zeros_like(rest)], axis=0)
        terms = dot(jnp.concatenate([terms, again], axis=1), weights, 1, 0)
        coefficients = terms[: len(pair) * sketch_rows] + terms[len(pair) * sketch_rows :]
        for side, slot in pair:
            a, b = slots[slot]
            i, j = place(slot)
            c = coefficients[side * sketch_rows : (side + 1) * sketch_rows]
            c_out[a, 0, b, 0] = c
            gain = fold(c * (products[side] + shifts[side] * c))
            residuals[slot] = norms[slot] - jnp.where(j < i, gain, 0.0)

    def norm_wait(ref):
        return pltpu.make_async_remote_copy(
            src_ref=ref,
            dst_ref=ref,
            send_sem=sem_ns,
            recv_sem=sem_nr,
            device_id=(p, sibling),
            device_id_type=MESH,
        )

    others = norm_wait(sums.at[pl.ds(0, devices - 1)])
    others.wait_recv()
    whole_out[...] = jnp.sum(sums[...], axis=0)
    others.wait_send()

    owns_points = q < 0
    for a in range(row_tiles):
        owns_points = owns_points | (lax.rem(a * rows + p, cols) == q)

    @pl.when(owns_points)
    def _():
        for target in point_targets:
            pl.when(wants_points(q, target))(point_copy(q, target).wait_send)

    for other, wanted in bank_steps:
        pl.when(wanted)(bank_copy(q, other, sem_br.at[q]).wait_send)
    pl.when(beside)(bank_copy(0, sibling, sem_sr, cols // 2).wait_send)


def finish(rows, cols, row_tiles, col_tiles, y, c, residuals, whole, y_out, c_out, err_out, rank_out, sems):
    p = lax.axis_index("prow")
    q = lax.axis_index("pcol")
    copies = [
        pltpu.make_async_copy(source.at[a], target.at[a], sems.at[index, a])
        for index, (source, target) in enumerate([(y, y_out), (c, c_out)])
        for a in range(row_tiles)
    ]
    for copy in copies:
        copy.start()
    norm = lax.rsqrt(all_sum(whole[0:1, :])) * float(cols * col_tiles)
    lane = lax.broadcasted_iota(jnp.int32, (1, 128), 1)
    for b in range(col_tiles):
        line = jnp.zeros((1, 128), F32)
        for a in range(row_tiles):
            error = jnp.sqrt(jnp.maximum(all_sum(residuals[a * col_tiles + b]), 0.0)) * norm
            shown = (lane == a) & (b * cols + q <= a * rows + p)
            line = jnp.where(shown, error, line)
        err_out[0, b, 0:1, :] = line[:, :row_tiles]
    rank_out[0] = whole[1:2, 0:1].astype(jnp.int32)[0, 0]
    for copy in copies:
        copy.wait()


def per_device(rows, cols, points, range_length, smoothness, bank, ids, ranks):
    row_tiles, col_tiles = ids.shape[0], ids.shape[2]
    per_bank, sketch_rows, size = bank.shape
    slots = row_tiles * col_tiles
    ids = ids.transpose(1, 2, 3, 0)
    ranks = ranks.transpose(1, 2, 3, 0)
    factors = jax.ShapeDtypeStruct((row_tiles, 1, col_tiles, 1, sketch_rows, size), F32)
    vmem = pl.BlockSpec(memory_space=pltpu.VMEM)
    smem = pl.BlockSpec(memory_space=pltpu.SMEM)
    hbm = pl.BlockSpec(memory_space=pltpu.HBM)
    dma = pltpu.SemaphoreType.DMA
    pinned = [pltpu.with_memory_space_constraint(x, pltpu.HBM) for x in (points, bank, ids, ranks)]
    y, c, residuals, whole = pl.pallas_call(
        functools.partial(kernel, rows, cols, row_tiles, col_tiles),
        out_shape=(
            factors,
            factors,
            jax.ShapeDtypeStruct((slots, 8, 128), F32),
            jax.ShapeDtypeStruct((2, 128), F32),
        ),
        in_specs=[smem, smem, hbm, hbm, hbm, hbm],
        out_specs=(vmem,) * 4,
        scratch_shapes=[
            pltpu.SMEM(ids.shape, jnp.int32),
            pltpu.SMEM(ranks.shape, jnp.int32),
            pltpu.VMEM((cols, col_tiles, 2, size), F32),
            pltpu.VMEM((cols * per_bank, sketch_rows, size), BF16),
            pltpu.VMEM((slots, size, size), BF16),
            pltpu.VMEM((slots, 8, 128), F32),
            pltpu.VMEM((col_tiles, size, 128), F32),
            pltpu.VMEM((col_tiles, size, 128), F32),
            pltpu.VMEM((2, size), F32),
            pltpu.VMEM((2, 128), F32),
            pltpu.VMEM((rows * cols, 2, 128), F32),
            dma((4,)),
            dma,
            dma((cols,)),
            dma,
            dma((cols,)),
            dma,
            dma,
            dma,
            pltpu.SemaphoreType.REGULAR,
        ],
        compiler_params=pltpu.CompilerParams(
            collective_id=0, has_side_effects=True, vmem_limit_bytes=40 * 1024 * 1024
        ),
        name="tiles",
    )(range_length, smoothness, *pinned)
    y, c, errors, rank_total = pl.pallas_call(
        functools.partial(finish, rows, cols, row_tiles, col_tiles),
        out_shape=(
            factors,
            factors,
            jax.ShapeDtypeStruct((1, col_tiles, 1, row_tiles), F32),
            jax.ShapeDtypeStruct((1,), jnp.int32),
        ),
        in_specs=[vmem] * 4,
        out_specs=(hbm, hbm, vmem, smem),
        scratch_shapes=[dma((2, row_tiles))],
        compiler_params=pltpu.CompilerParams(vmem_limit_bytes=16 * 1024 * 1024),
        name="finish",
    )(y, c, residuals, whole)
    return y, c, errors.transpose(3, 0, 1, 2), rank_total


def solution(mesh):
    in_specs = (
        P(None, "pcol", None, None),
        P(),
        P(),
        P("pcol", None, None),
        P(None, "prow", None, "pcol"),
        P(None, "prow", None, "pcol"),
    )
    out_specs = (
        P(None, "prow", None, "pcol", None, None),
        P(None, "prow", None, "pcol", None, None),
        P(None, "prow", None, "pcol"),
        P(),
    )
    return jax.shard_map(
        functools.partial(per_device, mesh.shape["prow"], mesh.shape["pcol"]),
        mesh=mesh,
        in_specs=in_specs,
        out_specs=out_specs,
        check_vma=False,
    )
```

```python
import functools
import math

import jax
import jax.numpy as jnp
from jax import lax
from jax.experimental import pallas as pl
from jax.experimental.pallas import tpu as pltpu
from jax.sharding import PartitionSpec as P

MESH = pl.DeviceIdType.MESH
LOG2E = math.log2(math.e)
F32 = jnp.float32
BF16 = jnp.bfloat16
HIGH = lax.Precision.HIGHEST


def dot(a, b, da, db, precision=None):
    return lax.dot_general(
        a, b, (((da,), (db,)), ((), ())), preferred_element_type=F32, precision=precision
    )


def split(x):
    high = x.astype(BF16)
    return high, (x - high.astype(F32)).astype(BF16)


def all_sum(x):
    return jnp.sum(jnp.sum(x, axis=1, keepdims=True), axis=0, keepdims=True)


def invert(m, size, half, group=8):
    parts = size // 8
    width = m.shape[1]
    sub = lax.broadcasted_iota(jnp.int32, (8, width), 0)
    lane = lax.broadcasted_iota(jnp.int32, (8, width), 1)
    side = lane // half * half
    lane = lane - side
    m = [m[8 * v : 8 * v + 8] for v in range(parts)]
    for start in range(0, size, group):
        cols = {
            k: [jnp.take_along_axis(part, side + k, axis=1) for part in m]
            for k in range(start, start + group)
        }
        for k in range(start, start + group):
            at, within = divmod(k, 8)
            col = cols.pop(k)
            pivot = jnp.broadcast_to(col[at][within : within + 1], (8, width))
            inverse = 1.0 / pivot
            for other, entry in cols.items():
                head = jnp.broadcast_to(entry[at][within : within + 1], (8, width)) * inverse
                entry = [e - c * head for e, c in zip(entry, col)]
                entry[at] = jnp.where(sub == within, head, entry[at])
                cols[other] = entry
            row = jnp.broadcast_to(m[at][within : within + 1], (8, width))
            row = jnp.where(lane == k, 1.0, row) * inverse
            m = [jnp.where(lane == k, 0.0, part) - c * row for part, c in zip(m, col)]
            m[at] = jnp.where(sub == within, row, m[at])
    return jnp.concatenate(m, axis=0)


def fold(x):
    rows, width = x.shape
    x = jnp.sum(x.reshape(rows // 8, 8, width), axis=0)
    return functools.reduce(jnp.add, [x[:, n : n + 128] for n in range(0, width, 128)])


def kernel(
    rows,
    cols,
    row_tiles,
    col_tiles,
    range_length,
    smoothness,
    points_hbm,
    bank_hbm,
    ids_hbm,
    ranks_hbm,
    y_out,
    c_out,
    residuals,
    whole_out,
    ids,
    ranks,
    all_points,
    all_bank,
    low,
    norms,
    x_spread,
    y_spread,
    line,
    mine,
    sums,
    sem_local,
    sem_ps,
    sem_pr,
    sem_bs,
    sem_br,
    sem_sr,
    sem_ns,
    sem_nr,
    ready,
):
    p = lax.axis_index("prow")
    q = lax.axis_index("pcol")
    per_bank, sketch_rows, size = bank_hbm.shape
    slots = [(a, b) for a in range(row_tiles) for b in range(col_tiles)]
    sibling = q + 1 - 2 * lax.rem(q, 2)
    mirrored = row_tiles == 2 and col_tiles == 1 and cols == 2 * rows

    barrier = pltpu.get_barrier_semaphore()
    for step in range(1, cols):
        pl.semaphore_signal(
            barrier, device_id=(p, lax.rem(q + step, cols)), device_id_type=MESH
        )
    gate = q == 0

    def tell_gates(semaphore):
        for step in range(1, rows):
            pl.semaphore_signal(
                semaphore, device_id=(lax.rem(p + step, rows), 0), device_id_type=MESH
            )

    @pl.when(gate)
    def _():
        tell_gates(barrier)

    own_bank = pl.ds(q * per_bank, per_bank)
    local = [
        pltpu.make_async_copy(source, target, sem_local.at[index])
        for index, (source, target) in enumerate(
            [
                (points_hbm.at[:, 0], all_points.at[q]),
                (bank_hbm, all_bank.at[own_bank]),
                (ids_hbm, ids),
                (ranks_hbm, ranks),
            ]
        )
    ]
    for copy in local:
        copy.start()
    def place(slot):
        a, b = slots[slot]
        return a * rows + p, b * cols + q

    def wants_bank(device):
        wanted = device < 0
        for a, b in slots:
            wanted = wanted | (b * cols + device < a * rows + p)
        return wanted

    def wants_points(source, target):
        if mirrored:
            early = (source == p) & ((target < p) | (target >= p + rows))
            return early | ((source == p + rows) & (target < source))
        wanted = source < 0
        for a in range(row_tiles):
            wanted = wanted | (lax.rem(a * rows + p, cols) == source)
        return wanted

    bank_steps = []
    turned = q + 2 - 4 * lax.rem(q // 2, 2)
    nearest = [turned] + [lax.rem(q + step, cols) for step in range(4, cols, 4)]
    farther = [lax.rem(turned + step, cols) for step in range(4, cols, 4)]
    for other in nearest + farther:
        twin = other + 1 - 2 * lax.rem(other, 2)
        bank_steps.append((other, wants_bank(other) | wants_bank(twin)))
    here, beside = wants_bank(q), wants_bank(sibling)

    def clear(slot):
        norms[slot] = jnp.zeros((8, 128), F32)

        def chunk(c, _):
            low[slot, pl.ds(pl.multiple_of(c * 128, 128), 128)] = jnp.zeros((128, size), BF16)
            return 0

        lax.fori_loop(0, size // 128, chunk, 0)

    for slot in range(len(slots)):
        i, j = place(slot)
        pl.when(j > i)(functools.partial(clear, slot))

        @pl.when(j >= i)
        def _():
            a, b = slots[slot]
            y_out[a, 0, b, 0] = jnp.zeros((sketch_rows, size), F32)
    for copy in local:
        copy.wait()

    def point_copy(source, target):
        return pltpu.make_async_remote_copy(
            src_ref=all_points.at[source],
            dst_ref=all_points.at[source],
            send_sem=sem_ps,
            recv_sem=sem_pr.at[source],
            device_id=(p, target),
            device_id_type=MESH,
        )

    def bank_copy(block, target, recv, count=1):
        at = pl.ds(block * per_bank, per_bank * count)
        return pltpu.make_async_remote_copy(
            src_ref=all_bank.at[at],
            dst_ref=all_bank.at[at],
            send_sem=sem_bs,
            recv_sem=recv,
            device_id=(p, target),
            device_id_type=MESH,
        )

    degree = jnp.full((8, 128), smoothness[0].astype(F32))
    scale = (LOG2E * jnp.sqrt(2.0 * degree + 1.0)) / jnp.full((8, 128), range_length[0])
    scale = scale[:1]
    linear, square = 1.0 / LOG2E, 1.0 / (3.0 * LOG2E * LOG2E)

    def by_order(zero, one, two):
        return jnp.where(smoothness[0] >= 2, two, jnp.where(smoothness[0] >= 1, one, zero)).astype(F32)

    offset = by_order(-38.0, -31.0, math.log2(square))
    first = by_order(0.0, linear * 2.0**31, linear / square)
    constant = by_order(2.0**38, 2.0**31, 1.0 / square)
    for b in range(col_tiles):
        for n in range(0, size, 128):
            cut = slice(n, n + 128)
            x_own = all_points[q, b, 0:1, cut] * scale
            y_own = all_points[q, b, 1:2, cut] * scale
            x_spread[b, cut] = jnp.broadcast_to(x_own, (128, 128)).T
            y_spread[b, cut] = jnp.broadcast_to(y_own, (128, 128)).T

    def generate(slot, begin=0, end=size // 128):
        i, j = place(slot)
        b = slots[slot][1]
        row_block, row_major = lax.rem(i, cols), i // cols
        for n in range(0, size, 128):
            cut = slice(n, n + 128)
            line[:, cut] = all_points[row_block, row_major, :, cut] * scale

        def chunk(c, total):
            at = pl.ds(pl.multiple_of(c * 128, 128), 128)
            x_own, y_own = x_spread[b, at], y_spread[b, at]
            for n in range(0, size, 128):
                cut = slice(n, n + 128)
                dx = x_own - line[0:1, cut]
                dy = y_own - line[1:2, cut]
                d2 = dx * dx + dy * dy
                t = d2 * lax.rsqrt(jnp.maximum(d2, 1e-30))
                tile = ((constant + t * (first + t)) * jnp.exp2(offset - t)).astype(BF16)
                low[slot, at, cut] = tile
                tile = tile.astype(F32)
                total = total + jnp.sum((tile * tile).reshape(16, 8, 128), axis=0)
            return total

        total = jnp.zeros((8, 128), F32) if begin == 0 else norms[slot]
        norms[slot] = lax.fori_loop(begin, end, chunk, total)

    i, j = place(0)
    pl.when((i == 0) & (j == 0))(functools.partial(generate, 0))

    pl.semaphore_wait(barrier, cols - 1 + jnp.where(gate, rows - 1, 0))

    point_targets = [lax.rem(q + cols - step, cols) for step in range(1, cols)]
    for target in point_targets:
        pl.when(wants_points(q, target))(point_copy(q, target).start)
    for other, wanted in bank_steps[: len(nearest)]:
        pl.when(wanted)(bank_copy(q, other, sem_br.at[q]).start)
    pl.when((q != p) & (q != p + rows))(lambda: pl.delay(800))
    for other, wanted in bank_steps[len(nearest) :]:
        pl.when(wanted)(bank_copy(q, other, sem_br.at[q]).start)
    pl.when(beside)(bank_copy(q, sibling, sem_sr).start)
    @pl.when(gate)
    def _():
        tell_gates(ready)

    def open_gate():
        pl.semaphore_wait(ready, rows - 1)
        for step in range(1, cols):
            pl.semaphore_signal(ready, device_id=(p, step), device_id_type=MESH)


    def forward():
        for other, _ in bank_steps:
            pl.when(here | beside)(bank_copy(other, q, sem_br.at[other]).wait_recv)
            pl.when(beside)(bank_copy(other, sibling, sem_sr).start)

    devices = rows * cols
    me = p * cols + q

    def norm_copy(target):
        return pltpu.make_async_remote_copy(
            src_ref=mine,
            dst_ref=sums.at[me],
            send_sem=sem_ns,
            recv_sem=sem_nr,
            device_id=(target // cols, lax.rem(target, cols)),
            device_id_type=MESH,
        )

    def send_norms(weights):
        norm_sum = jnp.zeros((8, 128), F32)
        rank_sum = jnp.float32(0)
        for slot, (a, b) in enumerate(slots):
            i, j = place(slot)
            norm_sum = norm_sum + weights[slot] * norms[slot]
            rank_sum = rank_sum + jnp.where(j < i, ranks[0, b, 0, a], 0).astype(F32)
        mine[0:1, :] = jnp.sum(norm_sum, axis=0, keepdims=True)
        mine[1:2, :] = jnp.full((1, 128), rank_sum)
        sums[me] = mine[...]
        pl.when(~gate)(functools.partial(pl.semaphore_wait, ready, 1))
        for step in range(1, devices):
            norm_copy(lax.rem(me + step, devices)).start()

    arrived = []

    def await_points(a, skip=None):
        owner = lax.rem(a * rows + p, cols)
        fresh = owner != q
        for before in arrived:
            fresh = fresh & (owner != lax.rem(before * rows + p, cols))
        arrived.append(a)

        fresh = fresh & wants_points(owner, q)

        @pl.when(fresh if skip is None else fresh & ~skip)
        def _():
            point_copy(owner, q).wait_recv()

    if mirrored:
        middle = size // 256
        both, lone = q <= p, (q > p) & (q <= p + rows)
        pl.when(q == p + rows)(functools.partial(generate, 1))
        await_points(0)
        corner = gate & (p == 0)
        pl.when(corner)(point_copy(rows, q).wait_recv)
        pl.when(corner)(functools.partial(generate, 1, 0, middle))
        pl.when(gate & (p > 0))(functools.partial(generate, 0, 0, middle))
        pl.when(gate)(open_gate)
        pl.when(gate & (p > 0))(functools.partial(generate, 0, middle))
        pl.when((both & ~gate) | (q >= p + rows))(functools.partial(generate, 0))
        await_points(1, corner)
        alone = lone & (q < p + rows)
        early = alone & (sibling == p)
        late = size * 3 // 512
        pl.when(alone)(functools.partial(generate, 1, 0, late))
        pl.when(early)(forward)
        pl.when(alone)(functools.partial(generate, 1, late))
        from_first = jnp.where((q < p) | (q >= p + rows), 2.0, jnp.where(q == p, 1.0, 0.0))
        from_second = jnp.where(lone, jnp.where(q < p + rows, 2.0, 1.0), 0.0)
        send_norms([from_first, from_second])
        quarter = size // 512
        pl.when(both & ~corner)(functools.partial(generate, 1, 0, quarter))
        pl.when(~early)(forward)
        pl.when(both & ~corner)(functools.partial(generate, 1, quarter))
        pl.when(corner)(functools.partial(generate, 1, middle))
    else:
        for slot, (a, b) in enumerate(slots):
            i, j = place(slot)
            if a not in arrived:
                await_points(a)
            pl.when((j <= i) & (i + j > 0) if slot == 0 else j <= i)(functools.partial(generate, slot))
        pl.when(gate)(open_gate)
        weights = []
        for slot in range(len(slots)):
            i, j = place(slot)
            weights.append(jnp.where(j < i, 2.0, 1.0))
        send_norms(weights)
        forward()

    pl.when(here)(bank_copy(0, q, sem_sr, cols // 2).wait_recv)

    half = 64
    row_at = lax.broadcasted_iota(jnp.int32, (sketch_rows, 1), 0)

    def rank_of(slot):
        a, b = slots[slot]
        i, j = place(slot)
        return jnp.where(j < i, ranks[0, b, 0, a], 0)

    def valid(slot):
        i, j = place(slot)
        return j < i

    def sketch_tile(slot):
        a, b = slots[slot]
        sketch = all_bank[ids[0, b, 0, a]]
        sketch = jnp.where(row_at < ranks[0, b, 0, a], sketch.astype(F32), 0.0).astype(BF16)
        y_out[a, 0, b, 0] = dot(sketch, low[slot], 1, 0)

    blank = jnp.zeros((half - sketch_rows, size), BF16)

    def stack(parts):
        full = [x for part in parts for x in (part, blank)]
        if len(parts) == 1:
            full += full[:1] + [blank]
        return jnp.concatenate(full, axis=0)

    for first in range(0, len(slots), 2):
        pair = list(enumerate(range(first, min(first + 2, len(slots)))))
        highs, lows = [], []
        wanted = [valid(slot) for _, slot in pair]
        every = functools.reduce(jnp.logical_and, wanted)

        @pl.when(every)
        def _():
            for _, slot in pair:
                sketch_tile(slot)

        for (_, slot), want in zip(pair, wanted):
            pl.when(want & ~every)(functools.partial(sketch_tile, slot))

        for side, slot in pair:
            a, b = slots[slot]
            high, rest = split(y_out[a, 0, b, 0])
            highs.append(high)
            lows.append(rest)
        high, rest = stack(highs), stack(lows)
        gram = dot(jnp.concatenate([high, rest], axis=0), high, 1, 1)
        gram = gram[: 2 * half] + gram[2 * half :] + dot(high, rest, 1, 1)
        lane = lax.broadcasted_iota(jnp.int32, (sketch_rows, 2 * half), 1)
        sub = lax.broadcasted_iota(jnp.int32, (sketch_rows, 2 * half), 0)
        left = lane < half
        gram = jnp.where(left, gram[:sketch_rows], gram[half : half + sketch_rows])
        eye = lane == jnp.where(left, sub, sub + half)
        shifts = []
        diagonal = jnp.ones((sketch_rows, 2 * half), F32)
        for side, slot in pair:
            a, b = slots[slot]
            mask = left if side == 0 else ~left
            rank = jnp.full((1, 1), ranks[0, b, 0, a].astype(F32))
            shift = 0.1 * all_sum(jnp.where(eye & mask, gram, 0.0)) / rank
            shifts.append(shift)
            diagonal = jnp.where(mask & (sub < rank_of(slot)), shift, diagonal)
        inverse = invert(gram + jnp.where(eye, diagonal, 0.0), sketch_rows, half)
        products, highs_w, lows_w = [], [], []
        for side, slot in pair:
            product = dot(jnp.concatenate([highs[side], lows[side]], axis=0), low[slot], 1, 1)
            high, rest = split(product[:sketch_rows])
            highs_w.append(high)
            lows_w.append(rest)
            products.append(product[:sketch_rows] + 2.0 * product[sketch_rows:])
        weights = jnp.concatenate([stack(highs_w), stack(lows_w)], axis=0)
        sides = [jnp.where(left if side == 0 else ~left, inverse, 0.0) for side, _ in pair]
        high, rest = split(jnp.concatenate(sides, axis=0))
        terms = jnp.concatenate([high, rest], axis=0)
        again = jnp.concatenate([high, jnp.zeros_like(rest)], axis=0)
        terms = dot(jnp.concatenate([terms, again], axis=1), weights, 1, 0)
        coefficients = terms[: len(pair) * sketch_rows] + terms[len(pair) * sketch_rows :]
        for side, slot in pair:
            a, b = slots[slot]
            i, j = place(slot)
            c = coefficients[side * sketch_rows : (side + 1) * sketch_rows]
            c_out[a, 0, b, 0] = c
            gain = fold(c * (products[side] + shifts[side] * c))
            residuals[slot] = norms[slot] - jnp.where(j < i, gain, 0.0)

    def norm_wait(ref):
        return pltpu.make_async_remote_copy(
            src_ref=ref,
            dst_ref=ref,
            send_sem=sem_ns,
            recv_sem=sem_nr,
            device_id=(p, sibling),
            device_id_type=MESH,
        )

    others = norm_wait(sums.at[pl.ds(0, devices - 1)])
    others.wait_recv()
    whole_out[...] = jnp.sum(sums[...], axis=0)
    others.wait_send()

    owns_points = q < 0
    for a in range(row_tiles):
        owns_points = owns_points | (lax.rem(a * rows + p, cols) == q)

    @pl.when(owns_points)
    def _():
        for target in point_targets:
            pl.when(wants_points(q, target))(point_copy(q, target).wait_send)

    for other, wanted in bank_steps:
        pl.when(wanted)(bank_copy(q, other, sem_br.at[q]).wait_send)
    pl.when(beside)(bank_copy(0, sibling, sem_sr, cols // 2).wait_send)


def finish(rows, cols, row_tiles, col_tiles, y, c, residuals, whole, y_out, c_out, err_out, rank_out, sems):
    p = lax.axis_index("prow")
    q = lax.axis_index("pcol")
    copies = [
        pltpu.make_async_copy(source.at[a], target.at[a], sems.at[index, a])
        for index, (source, target) in enumerate([(y, y_out), (c, c_out)])
        for a in range(row_tiles)
    ]
    for copy in copies:
        copy.start()
    norm = lax.rsqrt(all_sum(whole[0:1, :])) * float(cols * col_tiles)
    lane = lax.broadcasted_iota(jnp.int32, (1, 128), 1)
    for b in range(col_tiles):
        line = jnp.zeros((1, 128), F32)
        for a in range(row_tiles):
            error = jnp.sqrt(jnp.maximum(all_sum(residuals[a * col_tiles + b]), 0.0)) * norm
            shown = (lane == a) & (b * cols + q <= a * rows + p)
            line = jnp.where(shown, error, line)
        err_out[0, b, 0:1, :] = line[:, :row_tiles]
    rank_out[0] = whole[1:2, 0:1].astype(jnp.int32)[0, 0]
    for copy in copies:
        copy.wait()


def per_device(rows, cols, points, range_length, smoothness, bank, ids, ranks):
    row_tiles, col_tiles = ids.shape[0], ids.shape[2]
    per_bank, sketch_rows, size = bank.shape
    slots = row_tiles * col_tiles
    ids = ids.transpose(1, 2, 3, 0)
    ranks = ranks.transpose(1, 2, 3, 0)
    factors = jax.ShapeDtypeStruct((row_tiles, 1, col_tiles, 1, sketch_rows, size), F32)
    vmem = pl.BlockSpec(memory_space=pltpu.VMEM)
    smem = pl.BlockSpec(memory_space=pltpu.SMEM)
    hbm = pl.BlockSpec(memory_space=pltpu.HBM)
    dma = pltpu.SemaphoreType.DMA
    pinned = [pltpu.with_memory_space_constraint(x, pltpu.HBM) for x in (points, bank, ids, ranks)]
    y, c, residuals, whole = pl.pallas_call(
        functools.partial(kernel, rows, cols, row_tiles, col_tiles),
        out_shape=(
            factors,
            factors,
            jax.ShapeDtypeStruct((slots, 8, 128), F32),
            jax.ShapeDtypeStruct((2, 128), F32),
        ),
        in_specs=[smem, smem, hbm, hbm, hbm, hbm],
        out_specs=(vmem,) * 4,
        scratch_shapes=[
            pltpu.SMEM(ids.shape, jnp.int32),
            pltpu.SMEM(ranks.shape, jnp.int32),
            pltpu.VMEM((cols, col_tiles, 2, size), F32),
            pltpu.VMEM((cols * per_bank, sketch_rows, size), BF16),
            pltpu.VMEM((slots, size, size), BF16),
            pltpu.VMEM((slots, 8, 128), F32),
            pltpu.VMEM((col_tiles, size, 128), F32),
            pltpu.VMEM((col_tiles, size, 128), F32),
            pltpu.VMEM((2, size), F32),
            pltpu.VMEM((2, 128), F32),
            pltpu.VMEM((rows * cols, 2, 128), F32),
            dma((4,)),
            dma,
            dma((cols,)),
            dma,
            dma((cols,)),
            dma,
            dma,
            dma,
            pltpu.SemaphoreType.REGULAR,
        ],
        compiler_params=pltpu.CompilerParams(
            collective_id=0, has_side_effects=True, vmem_limit_bytes=40 * 1024 * 1024
        ),
        name="tiles",
    )(range_length, smoothness, *pinned)
    y, c, errors, rank_total = pl.pallas_call(
        functools.partial(finish, rows, cols, row_tiles, col_tiles),
        out_shape=(
            factors,
            factors,
            jax.ShapeDtypeStruct((1, col_tiles, 1, row_tiles), F32),
            jax.ShapeDtypeStruct((1,), jnp.int32),
        ),
        in_specs=[vmem] * 4,
        out_specs=(hbm, hbm, vmem, smem),
        scratch_shapes=[dma((2, row_tiles))],
        compiler_params=pltpu.CompilerParams(vmem_limit_bytes=16 * 1024 * 1024),
        name="finish",
    )(y, c, residuals, whole)
    return y, c, errors.transpose(3, 0, 1, 2), rank_total


def solution(mesh):
    in_specs = (
        P(None, "pcol", None, None),
        P(),
        P(),
        P("pcol", None, None),
        P(None, "prow", None, "pcol"),
        P(None, "prow", None, "pcol"),
    )
    out_specs = (
        P(None, "prow", None, "pcol", None, None),
        P(None, "prow", None, "pcol", None, None),
        P(None, "prow", None, "pcol"),
        P(),
    )
    return jax.shard_map(
        functools.partial(per_device, mesh.shape["prow"], mesh.shape["pcol"]),
        mesh=mesh,
        in_specs=in_specs,
        out_specs=out_specs,
        check_vma=False,
    )
```
